128 devices in a mesh: data: 1, fsdp: 2 (over core), ep: 64 (over z, y, x).
Axes of the slice: x: 4, y: 4, z: 4, core: 2. Of those that a mesh axis runs over, the one named last changes fastest.
Arguments:
- x_in: bfloat16 [128, 384, 2048], P(('data', 'fsdp', 'ep'))
- w_qkv: bfloat16 [2048, 6144], P('fsdp')
- w_out: bfloat16 [2048, 2048], P('fsdp')
- w_gate: bfloat16 [64, 2048, 1408], P('ep', 'fsdp')
- w_up: bfloat16 [64, 2048, 1408], P('ep', 'fsdp')
- w_down: bfloat16 [64, 1408, 2048], P('ep', None, 'fsdp')
- ws_gate: bfloat16 [2048, 2816], P('fsdp')
- ws_up: bfloat16 [2048, 2816], P('fsdp')
- ws_down: bfloat16 [2816, 2048], P(None, 'fsdp')
- expert_ids: int32 [128, 384, 6], P(('data', 'fsdp', 'ep'))
- slot_ids: int32 [128, 384, 6], P(('data', 'fsdp', 'ep'))
- gate_vals: bfloat16 [128, 384, 6], P(('data', 'fsdp', 'ep'))
Outputs:
- output: bfloat16 [128, 384, 2048], P(('data', 'fsdp', 'ep'))
All inputs are finite; a program needn't handle non-finite values.
Results may differ from the reference program's by a relative error of at most 0.00961563.
Values are sent between devices in bfloat16 or wider.
A program may use at most 1 GiB of HBM per device.

```python
import jax
import jax.numpy as jnp
from jax import lax

MODEL_DIM = 2048
NUM_HEADS = 16
HEAD_DIM = 128
NUM_EXPERTS = 64
TOP_K = 6
EXPERT_FF = 1408
SHARED_FF = 2816
BATCH_DEV = 1
SEQ_LEN = 384
GROUP_DEVS = 128
TOKENS = BATCH_DEV * SEQ_LEN
CAPACITY = ((5 * TOKENS * TOP_K) // (4 * NUM_EXPERTS) + 7) // 8 * 8
ROPE_BASE = 10000.0
EPSILON = 1e-6


def normal_weight(rand_key, weight_shape, fan_in):
    scaled = jax.random.normal(rand_key, weight_shape, jnp.float32) * (fan_in ** -0.5)
    return scaled.astype(jnp.bfloat16)


def draw_routing(rand_key):
    score_key, bias_key, hot_key = jax.random.split(rand_key, 3)
    expert_iota = jnp.arange(NUM_EXPERTS, dtype=jnp.int32)
    scores = jax.random.randint(score_key, (GROUP_DEVS, TOKENS, NUM_EXPERTS), 0, 1000, dtype=jnp.int32)
    expert_bias = jax.random.randint(bias_key, (GROUP_DEVS, 1, NUM_EXPERTS), 0, 500, dtype=jnp.int32)
    hot_expert = jax.random.randint(hot_key, (GROUP_DEVS, 1, 1), 0, NUM_EXPERTS, dtype=jnp.int32)
    total_score = scores + expert_bias + jnp.where(expert_iota == hot_expert, 2000, 0)
    ranked = total_score * NUM_EXPERTS + expert_iota
    chosen = lax.top_k(ranked, TOP_K)[1].astype(jnp.int32)
    flat_ids = chosen.reshape(GROUP_DEVS, TOKENS * TOP_K)

    def device_slots(dev_ids):
        onehot = (dev_ids[:, None] == expert_iota[None, :]).astype(jnp.int32)
        running = jnp.cumsum(onehot, axis=0) - 1
        position = jnp.sum(running * onehot, axis=1)
        return jnp.where(position < CAPACITY, position, -1)

    slot_table = lax.map(device_slots, flat_ids)
    route_shape = (GROUP_DEVS * BATCH_DEV, SEQ_LEN, TOP_K)
    return chosen.reshape(route_shape), slot_table.reshape(route_shape)


def setup_inputs(seed: int = 0, part: int = 0) -> dict:
    weight_keys = jax.random.split(jax.random.key(seed), 8)
    part_keys = jax.random.split(jax.random.fold_in(jax.random.key(seed + 1), part), 3)
    n_seqs = GROUP_DEVS * BATCH_DEV
    expert_ids, slot_ids = draw_routing(part_keys[1])
    x_in = jax.random.normal(part_keys[0], (n_seqs, SEQ_LEN, MODEL_DIM), jnp.float32).astype(jnp.bfloat16)
    gate_vals = jax.random.uniform(part_keys[2], (n_seqs, SEQ_LEN, TOP_K), jnp.float32, 0.25, 1.0).astype(jnp.bfloat16)
    return {"x_in": x_in, "w_qkv": normal_weight(weight_keys[0], (MODEL_DIM, 3 * NUM_HEADS * HEAD_DIM), MODEL_DIM), "w_out": normal_weight(weight_keys[1], (NUM_HEADS * HEAD_DIM, MODEL_DIM), NUM_HEADS * HEAD_DIM), "w_gate": normal_weight(weight_keys[2], (NUM_EXPERTS, MODEL_DIM, EXPERT_FF), MODEL_DIM), "w_up": normal_weight(weight_keys[3], (NUM_EXPERTS, MODEL_DIM, EXPERT_FF), MODEL_DIM), "w_down": normal_weight(weight_keys[4], (NUM_EXPERTS, EXPERT_FF, MODEL_DIM), EXPERT_FF), "ws_gate": normal_weight(weight_keys[5], (MODEL_DIM, SHARED_FF), MODEL_DIM), "ws_up": normal_weight(weight_keys[6], (MODEL_DIM, SHARED_FF), MODEL_DIM), "ws_down": normal_weight(weight_keys[7], (SHARED_FF, MODEL_DIM), SHARED_FF), "expert_ids": expert_ids, "slot_ids": slot_ids, "gate_vals": gate_vals}


def rms_norm(values):
    vals_f32 = values.astype(jnp.float32)
    mean_sq = jnp.mean(vals_f32 * vals_f32, axis=-1, keepdims=True)
    return (vals_f32 * lax.rsqrt(mean_sq + EPSILON)).astype(jnp.bfloat16)


def rotary_embed(heads_in, positions):
    half_dim = HEAD_DIM // 2
    inv_freq = ROPE_BASE ** (-jnp.arange(half_dim).astype(jnp.float32) * (2.0 / HEAD_DIM))
    angles = positions[:, None] * inv_freq[None, :]
    cos_tab = jnp.cos(angles)[:, None, :]
    sin_tab = jnp.sin(angles)[:, None, :]
    vals_f32 = heads_in.astype(jnp.float32)
    first_half = vals_f32[..., :half_dim]
    second_half = vals_f32[..., half_dim:]
    rotated = jnp.concatenate([first_half * cos_tab - second_half * sin_tab, second_half * cos_tab + first_half * sin_tab], axis=-1)
    return rotated.astype(jnp.bfloat16)


def attention_block(x_dev, w_qkv, w_out):
    normed = rms_norm(x_dev).reshape(TOKENS, MODEL_DIM)
    qkv_proj = jnp.dot(normed, w_qkv, preferred_element_type=jnp.float32).astype(jnp.bfloat16)
    qkv_proj = qkv_proj.reshape(BATCH_DEV, SEQ_LEN, 3, NUM_HEADS, HEAD_DIM)
    positions = jnp.arange(SEQ_LEN).astype(jnp.float32)
    query_rot = rotary_embed(qkv_proj[:, :, 0], positions).astype(jnp.float32)
    key_rot = rotary_embed(qkv_proj[:, :, 1], positions).astype(jnp.float32)
    value_heads = qkv_proj[:, :, 2].astype(jnp.float32)
    scores = jnp.einsum("bqhd,bkhd->bhqk", query_rot, key_rot) * (HEAD_DIM ** -0.5)
    causal = jnp.arange(SEQ_LEN)[:, None] >= jnp.arange(SEQ_LEN)[None, :]
    attn_probs = jax.nn.softmax(jnp.where(causal, scores, -1e30), axis=-1).astype(jnp.bfloat16)
    attn_mixed = jnp.einsum("bhqk,bkhd->bqhd", attn_probs.astype(jnp.float32), value_heads).astype(jnp.bfloat16)
    attn_out = jnp.dot(attn_mixed.reshape(TOKENS, NUM_HEADS * HEAD_DIM), w_out, preferred_element_type=jnp.float32)
    return (x_dev.reshape(TOKENS, MODEL_DIM).astype(jnp.float32) + attn_out).astype(jnp.bfloat16)


def expert_rows(operands):
    rows_in, gate_w, up_w, down_w = operands
    gate_act = jnp.dot(rows_in, gate_w, preferred_element_type=jnp.float32)
    up_act = jnp.dot(rows_in, up_w, preferred_element_type=jnp.float32)
    inner_act = (jax.nn.silu(gate_act) * up_act).astype(jnp.bfloat16)
    return jnp.dot(inner_act, down_w, preferred_element_type=jnp.float32).astype(jnp.bfloat16)


def moe_block(hidden, dev_ids, dev_slots, dev_gates, w_gate, w_up, w_down, ws_gate, ws_up, ws_down):
    normed = rms_norm(hidden)
    kept_mask = dev_slots >= 0
    row_index = dev_ids * CAPACITY + dev_slots
    target = jnp.where(kept_mask, row_index, NUM_EXPERTS * CAPACITY).reshape(-1)
    source_tok = jnp.arange(TOKENS * TOP_K, dtype=jnp.int32) // TOP_K
    row_source = jnp.full((NUM_EXPERTS * CAPACITY,), TOKENS, jnp.int32).at[target].set(source_tok, mode="drop")
    buffer = jnp.take(normed, row_source, axis=0, mode="fill", fill_value=0).reshape(NUM_EXPERTS, CAPACITY, MODEL_DIM)
    expert_out = lax.map(expert_rows, (buffer, w_gate, w_up, w_down)).reshape(NUM_EXPERTS * CAPACITY, MODEL_DIM)
    picked = jnp.take(expert_out, jnp.where(kept_mask, row_index, 0), axis=0).astype(jnp.float32)
    weight = jnp.where(kept_mask, dev_gates.astype(jnp.float32), 0.0)
    routed = jnp.sum(weight[:, :, None] * picked, axis=1)
    shared_act = jax.nn.silu(jnp.dot(normed, ws_gate, preferred_element_type=jnp.float32)) * jnp.dot(normed, ws_up, preferred_element_type=jnp.float32)
    shared_out = jnp.dot(shared_act.astype(jnp.bfloat16), ws_down, preferred_element_type=jnp.float32)
    return (hidden.astype(jnp.float32) + shared_out + routed).astype(jnp.bfloat16)


def reference(x_in, w_qkv, w_out, w_gate, w_up, w_down, ws_gate, ws_up, ws_down, expert_ids, slot_ids, gate_vals):
    def per_device(operands):
        x_dev, dev_ids, dev_slots, dev_gates = operands
        hidden = attention_block(x_dev, w_qkv, w_out)
        return moe_block(hidden, dev_ids, dev_slots, dev_gates, w_gate, w_up, w_down, ws_gate, ws_up, ws_down)

    stacked = (x_in.reshape(GROUP_DEVS, BATCH_DEV, SEQ_LEN, MODEL_DIM), expert_ids.reshape(GROUP_DEVS, TOKENS, TOP_K), slot_ids.reshape(GROUP_DEVS, TOKENS, TOP_K), gate_vals.reshape(GROUP_DEVS, TOKENS, TOP_K))
    out_rows = lax.map(per_device, stacked)
    return out_rows.reshape(GROUP_DEVS * BATCH_DEV, SEQ_LEN, MODEL_DIM)
```

```python
import jax
import jax.numpy as jnp
from jax import lax
from jax.sharding import PartitionSpec as P

HEAD_DIM = 128
ROPE_BASE = 10000.0
EPSILON = 1e-6


def rms_norm(values):
    vals_f32 = values.astype(jnp.float32)
    mean_sq = jnp.mean(vals_f32 * vals_f32, axis=-1, keepdims=True)
    return (vals_f32 * lax.rsqrt(mean_sq + EPSILON)).astype(jnp.bfloat16)


def rotary_embed(heads_in, positions):
    half_dim = HEAD_DIM // 2
    inv_freq = ROPE_BASE ** (-jnp.arange(half_dim, dtype=jnp.float32) * (2.0 / HEAD_DIM))
    angles = positions[:, None] * inv_freq[None, :]
    cos_tab = jnp.cos(angles)[:, None, :]
    sin_tab = jnp.sin(angles)[:, None, :]
    vals_f32 = heads_in.astype(jnp.float32)
    first_half = vals_f32[..., :half_dim]
    second_half = vals_f32[..., half_dim:]
    rotated = jnp.concatenate([first_half * cos_tab - second_half * sin_tab, second_half * cos_tab + first_half * sin_tab], axis=-1)
    return rotated.astype(jnp.bfloat16)


def dot32(left, right):
    return jnp.dot(left, right, preferred_element_type=jnp.float32)


def split_cols(values, fs):
    half = values.shape[-1] // 2
    own = lax.dynamic_slice_in_dim(values, fs * half, half, axis=values.ndim - 1)
    other = lax.dynamic_slice_in_dim(values, (1 - fs) * half, half, axis=values.ndim - 1)
    return own, other


def paired_dot(own_other, pair):
    return dot32(own_other[0], pair[0]) + dot32(own_other[1], pair[1])


def join_cols(left, pair, fs):
    own, other = dot32(left, pair[0]), dot32(left, pair[1])
    return jnp.where(fs == 0, jnp.concatenate([own, other], axis=1), jnp.concatenate([other, own], axis=1))


def attention_block(x_in, qkv_pair, out_pair, fs):
    n_batch, seq_len, model_dim = x_in.shape
    n_heads = qkv_pair[0].shape[1] // (3 * HEAD_DIM)
    normed = rms_norm(x_in).reshape(n_batch * seq_len, model_dim)
    qkv_proj = paired_dot(split_cols(normed, fs), qkv_pair).astype(jnp.bfloat16)
    qkv_proj = qkv_proj.reshape(n_batch, seq_len, 3, n_heads, HEAD_DIM)
    positions = jnp.arange(seq_len, dtype=jnp.float32)
    query_rot = rotary_embed(qkv_proj[:, :, 0], positions)
    key_rot = rotary_embed(qkv_proj[:, :, 1], positions)
    scores = jnp.einsum("bqhd,bkhd->bhqk", query_rot, key_rot, preferred_element_type=jnp.float32) * (HEAD_DIM ** -0.5)
    causal = jnp.arange(seq_len)[:, None] >= jnp.arange(seq_len)[None, :]
    attn_probs = jax.nn.softmax(jnp.where(causal, scores, -1e30), axis=-1).astype(jnp.bfloat16)
    attn_mixed = jnp.einsum("bhqk,bkhd->bqhd", attn_probs, qkv_proj[:, :, 2], preferred_element_type=jnp.float32).astype(jnp.bfloat16)
    mixed = split_cols(attn_mixed.reshape(n_batch * seq_len, n_heads * HEAD_DIM), fs)
    return (x_in.reshape(n_batch * seq_len, model_dim).astype(jnp.float32) + paired_dot(mixed, out_pair)).astype(jnp.bfloat16)


def capacity_for(n_tokens, top_k, n_experts):
    return ((5 * n_tokens * top_k) // (4 * n_experts) + 7) // 8 * 8


def solution(mesh):
    n_ep = mesh.shape["ep"]
    tok_spec = P(("data", "fsdp", "ep"))
    row_spec = P("fsdp", None)

    def local_step(x_in, w_qkv, w_out, w_gate, w_up, w_down, ws_gate, ws_up, ws_down, expert_ids, slot_ids, gate_vals):
        n_batch, seq_len, model_dim = x_in.shape
        n_tokens = n_batch * seq_len
        top_k = expert_ids.shape[-1]
        n_experts = w_gate.shape[0] * n_ep
        capacity = capacity_for(n_tokens, top_k, n_experts)
        n_rows = n_experts * capacity
        fs = lax.axis_index("fsdp")

        def paired(weight):
            return weight, lax.ppermute(weight, "fsdp", [(0, 1), (1, 0)])

        qkv_pair, out_pair = paired(w_qkv), paired(w_out)
        gate_pair, up_pair, down_pair = paired(w_gate[0]), paired(w_up[0]), paired(w_down[0])
        sgate_pair, sup_pair, sdown_pair = paired(ws_gate), paired(ws_up), paired(ws_down)

        ids_flat = expert_ids.reshape(n_tokens, top_k)
        slots_flat = slot_ids.reshape(n_tokens, top_k)
        row_of = jnp.where(slots_flat >= 0, ids_flat * capacity + slots_flat, -1)
        row_iota = jnp.arange(n_rows, dtype=jnp.int32)
        gates = gate_vals.reshape(n_tokens, top_k)
        picks = sum((row_iota[:, None] == row_of[None, :, k]).astype(jnp.bfloat16) for k in range(top_k))
        spread = sum(jnp.where(row_of[:, k, None] == row_iota[None, :], gates[:, k, None], jnp.bfloat16(0)) for k in range(top_k))

        hidden = attention_block(x_in, qkv_pair, out_pair, fs)
        normed = rms_norm(hidden)
        buffer = dot32(picks, normed).astype(jnp.bfloat16).reshape(n_experts, capacity, model_dim)
        received = lax.all_to_all(buffer, "ep", 0, 0, tiled=True).reshape(n_rows, model_dim)

        halves = split_cols(normed, fs)
        shared_act = (jax.nn.silu(paired_dot(halves, sgate_pair)) * paired_dot(halves, sup_pair)).astype(jnp.bfloat16)
        base = hidden.astype(jnp.float32) + join_cols(shared_act, sdown_pair, fs)

        got = split_cols(received, fs)
        act = (jax.nn.silu(paired_dot(got, gate_pair)) * paired_dot(got, up_pair)).astype(jnp.bfloat16)
        expert_out = join_cols(act, down_pair, fs).astype(jnp.bfloat16).reshape(n_experts, capacity, model_dim)
        returned = lax.all_to_all(expert_out, "ep", 0, 0, tiled=True).reshape(n_rows, model_dim)
        summed = base + dot32(spread, returned)
        return summed.astype(jnp.bfloat16).reshape(n_batch, seq_len, model_dim)

    return jax.shard_map(local_step, mesh=mesh, in_specs=(tok_spec, row_spec, row_spec, P("ep", "fsdp", None), P("ep", "fsdp", None), P("ep", None, "fsdp"), row_spec, row_spec, P(None, "fsdp"), tok_spec, tok_spec, tok_spec), out_specs=tok_spec, check_vma=False)
```

```python
import functools

import jax
import jax.numpy as jnp
from jax import lax
from jax.experimental import pallas as pl
from jax.experimental.pallas import tpu as pltpu
from jax.sharding import PartitionSpec as P

HEAD_DIM = 128
ROPE_BASE = 10000.0
EPSILON = 1e-6
RING = 4
BLOCK = 8
TURNS = 3
WIDE = 256
MESH = pl.DeviceIdType.MESH
STRIDES = (RING * RING, RING, 1)


def rms_norm(values):
    vals_f32 = values.astype(jnp.float32)
    mean_sq = jnp.mean(vals_f32 * vals_f32, axis=-1, keepdims=True)
    return (vals_f32 * lax.rsqrt(mean_sq + EPSILON)).astype(jnp.bfloat16)


def rotary_embed(heads_in, positions):
    half_dim = HEAD_DIM // 2
    inv_freq = ROPE_BASE ** (-jnp.arange(half_dim, dtype=jnp.float32) * (2.0 / HEAD_DIM))
    angles = positions[:, None] * inv_freq[None, :]
    cos_tab = jnp.cos(angles)[:, None, :]
    sin_tab = jnp.sin(angles)[:, None, :]
    vals_f32 = heads_in.astype(jnp.float32)
    first_half = vals_f32[..., :half_dim]
    second_half = vals_f32[..., half_dim:]
    rotated = jnp.concatenate([first_half * cos_tab - second_half * sin_tab, second_half * cos_tab + first_half * sin_tab], axis=-1)
    return rotated.astype(jnp.bfloat16)


def dot32(left, right):
    return jnp.dot(left, right, preferred_element_type=jnp.float32)


def split_cols(values, fs):
    half = values.shape[-1] // 2
    own = lax.dynamic_slice_in_dim(values, fs * half, half, axis=values.ndim - 1)
    other = lax.dynamic_slice_in_dim(values, (1 - fs) * half, half, axis=values.ndim - 1)
    return own, other


def paired_dot(own_other, pair):
    return dot32(own_other[0], pair[0]) + dot32(own_other[1], pair[1])


def join_cols(left, pair, fs):
    own, other = dot32(left, pair[0]), dot32(left, pair[1])
    return jnp.where(fs == 0, jnp.concatenate([own, other], axis=1), jnp.concatenate([other, own], axis=1))


def attention_block(x_in, qkv_pair, out_pair, fs):
    n_batch, seq_len, model_dim = x_in.shape
    n_heads = qkv_pair[0].shape[1] // (3 * HEAD_DIM)
    normed = rms_norm(x_in).reshape(n_batch * seq_len, model_dim)
    qkv_proj = paired_dot(split_cols(normed, fs), qkv_pair).astype(jnp.bfloat16)
    qkv_proj = qkv_proj.reshape(n_batch, seq_len, 3, n_heads, HEAD_DIM)
    positions = jnp.arange(seq_len, dtype=jnp.float32)
    query_rot = rotary_embed(qkv_proj[:, :, 0], positions)
    key_rot = rotary_embed(qkv_proj[:, :, 1], positions)
    scores = jnp.einsum("bqhd,bkhd->bhqk", query_rot, key_rot, preferred_element_type=jnp.float32) * (HEAD_DIM ** -0.5)
    causal = jnp.arange(seq_len)[:, None] >= jnp.arange(seq_len)[None, :]
    attn_probs = jax.nn.softmax(jnp.where(causal, scores, -1e30), axis=-1).astype(jnp.bfloat16)
    attn_mixed = jnp.einsum("bhqk,bkhd->bqhd", attn_probs, qkv_proj[:, :, 2], preferred_element_type=jnp.float32).astype(jnp.bfloat16)
    mixed = split_cols(attn_mixed.reshape(n_batch * seq_len, n_heads * HEAD_DIM), fs)
    return (x_in.reshape(n_batch * seq_len, model_dim).astype(jnp.float32) + paired_dot(mixed, out_pair)).astype(jnp.bfloat16)


def capacity_for(n_tokens, top_k, n_experts):
    return ((5 * n_tokens * top_k) // (4 * n_experts) + 7) // 8 * 8


def ring_peer(me, axis, offset):
    stride = STRIDES[axis]
    place = lax.rem(me // stride, RING)
    return me + (lax.rem(place + offset + RING, RING) - place) * stride


class Exchange:
    def __init__(self, me, axes, sign, first, second, third, last, send, recv):
        self.me, self.axes, self.sign = me, axes, sign
        self.first, self.second, self.third, self.last = first, second, third, last
        self.send, self.recv = send, recv

    def push(self, phase, step, pairs):
        peer = ring_peer(self.me, self.axes[phase], self.sign * step)
        for src, dst in pairs:
            pltpu.make_async_remote_copy(src_ref=src, dst_ref=dst, send_sem=self.send.at[phase], recv_sem=self.recv.at[phase],
                                         device_id={"ep": peer}, device_id_type=MESH).start()

    def start(self, phase):
        for d in (1, 3, 2):
            if phase == 0:
                pairs = [(self.first.at[d], self.second.at[:, :, d - 1])]
            elif phase == 1:
                pairs = [(self.first.at[0, d], self.third.at[:, d - 1, 0]), (self.second.at[d], self.third.at[:, d - 1, pl.ds(1, 3)])]
            else:
                pairs = [(self.first.at[0, 0, d], self.last.at[d - 1, 0, 0]), (self.second.at[0, d], self.last.at[d - 1, 0, pl.ds(1, 3)]),
                         (self.third.at[d], self.last.at[d - 1, pl.ds(1, 3)])]
            self.push(phase, d, pairs)

    def landing(self, phase):
        return (self.second, self.third, self.last)[phase]

    def wait_recv(self, phase):
        whole = self.landing(phase)
        pltpu.make_async_copy(whole, whole, self.recv.at[phase]).wait()

    def wait_send(self, phase):
        whole = self.landing(phase)
        pltpu.make_async_copy(whole, whole, self.send.at[phase]).wait()

    def kept(self):
        return [(self.third.at[0], (0, pl.ds(1, 3))), (self.second.at[0, 0], (0, 0, pl.ds(1, 3))), (self.first.at[0, 0, 0], (0, 0, 0))]


def moe_kernel(n_units, rows_hbm, gate_a, gate_b, up_a, up_b, down_a, down_b, done_hbm,
               out1, out2, out3, made_hbm, back1, back2,
               ga, gb, ua, ub, da, db, x_ref, act_ref, y_ref, w_sem, x_sem, y_sem, fill_sem, go_send, go_recv, come_send, come_recv):
    me = lax.axis_index("ep")
    fs = lax.axis_index("fsdp")
    barrier = pltpu.get_barrier_semaphore()
    for axis in range(3):
        for d in range(1, RING):
            pl.semaphore_signal(barrier, inc=1, device_id={"ep": ring_peer(me, axis, d)}, device_id_type=MESH)
    pl.semaphore_wait(barrier, 3 * (RING - 1))

    half = ga.shape[0]
    inner = ga.shape[1]
    rows = RING ** 3 * BLOCK
    go, come = [], []
    for u in range(n_units):
        axes = tuple((u % TURNS + k) % 3 for k in range(3))
        go.append(Exchange(me, axes, 1, rows_hbm.at[u], out1.at[u], out2.at[u], out3.at[u], go_send.at[u], go_recv.at[u]))
        come.append(Exchange(me, axes[::-1], -1, made_hbm.at[u], back1.at[u], back2.at[u], done_hbm.at[u, pl.ds(1, 3)], come_send.at[u], come_recv.at[u]))
    batches = [range(b * TURNS, (b + 1) * TURNS) for b in range(n_units // TURNS)]

    for units in batches:
        for u in units:
            go[u].start(0)
    weights = [pltpu.make_async_copy(src, dst, w_sem.at[n]) for n, (src, dst) in enumerate(
        ((gate_a, ga), (gate_b, gb), (up_a, ua), (up_b, ub), (down_a, da), (down_b, db)))]
    for copy in weights:
        copy.start()
    for phase in range(2):
        for units in batches:
            for u in units:
                go[u].wait_recv(phase)
                go[u].start(phase + 1)
    for copy in weights:
        copy.wait()

    def x_copies(u):
        slot = u % 2
        pieces = [(go[u].last, (pl.ds(1, 3),))] + go[u].kept()
        return [pltpu.make_async_copy(src, x_ref.at[(slot, *place)], x_sem.at[slot, n]) for n, (src, place) in enumerate(pieces)]

    def y_copy(u):
        return pltpu.make_async_copy(y_ref.at[u % 2], made_hbm.at[u], y_sem.at[u % 2])

    def fetch(u):
        go[u].wait_recv(2)
        for copy in x_copies(u):
            copy.start()

    def expert(u):
        slot = u % 2
        x2 = x_ref.at[slot].reshape(rows, 2 * half)
        y2 = y_ref.at[slot].reshape(rows, 2 * half)

        def own(side):
            return pl.ds(pl.multiple_of(lax.rem(fs + side, 2) * half, half), half)

        def inner_block(cols):
            gate = dot32(x2[:, own(0)], ga[:, cols]) + dot32(x2[:, own(1)], gb[:, cols])
            up = dot32(x2[:, own(0)], ua[:, cols]) + dot32(x2[:, own(1)], ub[:, cols])
            act_ref[:, cols] = (jax.nn.silu(gate) * up).astype(jnp.bfloat16)

        def inner_step(n, carry):
            inner_block(pl.ds(pl.multiple_of(n * WIDE, WIDE), WIDE))
            return carry

        whole = inner // WIDE
        lax.fori_loop(0, whole, inner_step, 0)
        if inner % WIDE:
            inner_block(pl.ds(whole * WIDE, inner % WIDE))

        def down_step(n, carry):
            cols = pl.ds(pl.multiple_of(n * WIDE, WIDE), WIDE)
            for side, weight in enumerate((da, db)):
                target = pl.ds(pl.multiple_of(lax.rem(fs + side, 2) * half + n * WIDE, WIDE), WIDE)
                y2[:, target] = dot32(act_ref[...], weight[:, cols]).astype(jnp.bfloat16)
            return carry

        lax.fori_loop(0, half // WIDE, down_step, 0)

    fetch(0)
    for u in range(n_units):
        for copy in x_copies(u):
            copy.wait()
        if u + 1 < n_units:
            fetch(u + 1)
        if u >= 2:
            pass
        expert(u)
        y_copy(u).start()
        y_copy(u).wait()
        come[u].start(0)
    for phase in range(2):
        for units in batches:
            for u in units:
                come[u].wait_recv(phase)
                come[u].start(phase + 1)

    def fill(u):
        slot = u % 2
        return [(pltpu.make_async_copy(src, x_ref.at[(slot, *place)], fill_sem.at[slot, n]),
                 pltpu.make_async_copy(x_ref.at[(slot, *place)], done_hbm.at[(u, *place)], fill_sem.at[slot, n])) for n, (src, place) in enumerate(come[u].kept())]

    for u in range(n_units):
        copies = fill(u)
        for load, _ in copies:
            load.start()
        for load, store in copies:
            load.wait()
            store.start()
        for _, store in copies:
            store.wait()
    for u in range(n_units):
        come[u].wait_recv(2)
    for u in range(n_units):
        for phase in range(3):
            go[u].wait_send(phase)
            come[u].wait_send(phase)


def moe_exchange(rows, gate_pair, up_pair, down_pair):
    n_units, width = rows.shape[0], rows.shape[-1]
    anywhere = pl.BlockSpec(memory_space=pl.ANY)
    weights = (*gate_pair, *up_pair, *down_pair)
    inner = gate_pair[0].shape[1]

    def blocks(*lead):
        return jax.ShapeDtypeStruct((n_units, *lead, BLOCK, width), jnp.bfloat16)

    cube = (RING, RING, RING, BLOCK, width)
    outs = (blocks(4, 4, 4), blocks(4, 4, 3), blocks(4, 3, 4), blocks(3, 4, 4), blocks(4, 4, 4), blocks(4, 4, 3), blocks(4, 3, 4))
    sems = pltpu.SemaphoreType.DMA
    return pl.pallas_call(
        functools.partial(moe_kernel, n_units),
        out_shape=outs,
        in_specs=[anywhere] * 7,
        out_specs=(anywhere,) * 7,
        scratch_shapes=[pltpu.VMEM(w.shape, jnp.bfloat16) for w in weights] + [
            pltpu.VMEM((2, *cube), jnp.bfloat16),
            pltpu.VMEM((RING ** 3 * BLOCK, inner), jnp.bfloat16),
            pltpu.VMEM((2, *cube), jnp.bfloat16),
            sems((6,)), sems((2, 4)), sems((2,)), sems((2, 3)),
            sems((n_units, 3)), sems((n_units, 3)), sems((n_units, 3)), sems((n_units, 3)),
        ],
        compiler_params=pltpu.CompilerParams(collective_id=0, has_side_effects=True, vmem_limit_bytes=48 * 1024 * 1024),
        cost_estimate=pl.CostEstimate(flops=250_000_000_000, bytes_accessed=100_000_000, transcendentals=0),
        name="moe_exchange",
    )(rows, *weights)[0]


def solution(mesh):
    n_ep = mesh.shape["ep"]
    tok_spec = P(("data", "fsdp", "ep"))
    row_spec = P("fsdp", None)

    def local_step(x_in, w_qkv, w_out, w_gate, w_up, w_down, ws_gate, ws_up, ws_down, expert_ids, slot_ids, gate_vals):
        n_batch, seq_len, model_dim = x_in.shape
        n_tokens = n_batch * seq_len
        top_k = expert_ids.shape[-1]
        n_experts = w_gate.shape[0] * n_ep
        capacity = capacity_for(n_tokens, top_k, n_experts)
        n_rows = n_experts * capacity
        fs = lax.axis_index("fsdp")

        def paired(weight):
            return weight, lax.ppermute(weight, "fsdp", [(0, 1), (1, 0)])

        qkv_pair, out_pair = paired(w_qkv), paired(w_out)
        gate_pair, up_pair, down_pair = paired(w_gate[0]), paired(w_up[0]), paired(w_down[0])
        sgate_pair, sup_pair, sdown_pair = paired(ws_gate), paired(ws_up), paired(ws_down)

        ids_flat = expert_ids.reshape(n_tokens, top_k)
        slots_flat = slot_ids.reshape(n_tokens, top_k)
        me = lax.axis_index("ep")
        rel = [lax.rem(ids_flat // s - me // s + n_ep, RING) for s in STRIDES]
        unit, within = slots_flat // BLOCK, slots_flat % BLOCK
        turn = unit % TURNS
        place = jnp.zeros_like(slots_flat)
        for r in range(TURNS):
            order = [rel[(r + k) % 3] for k in range(3)]
            place = jnp.where(turn == r, (order[0] * RING + order[1]) * RING + order[2], place)
        row_of = jnp.where(slots_flat >= 0, (unit * n_experts + place) * BLOCK + within, -1)
        row_iota = jnp.arange(n_rows, dtype=jnp.int32)
        gates = gate_vals.reshape(n_tokens, top_k)
        picks = sum((row_iota[:, None] == row_of[None, :, k]).astype(jnp.bfloat16) for k in range(top_k))
        spread = sum(jnp.where(row_of[:, k, None] == row_iota[None, :], gates[:, k, None], jnp.bfloat16(0)) for k in range(top_k))

        hidden = attention_block(x_in, qkv_pair, out_pair, fs)
        normed = rms_norm(hidden)
        buffer = dot32(picks, normed).astype(jnp.bfloat16)
        rows = buffer.reshape(capacity // BLOCK, RING, RING, RING, BLOCK, model_dim)

        halves = split_cols(normed, fs)
        shared_act = (jax.nn.silu(paired_dot(halves, sgate_pair)) * paired_dot(halves, sup_pair)).astype(jnp.bfloat16)
        base = hidden.astype(jnp.float32) + join_cols(shared_act, sdown_pair, fs)

        returned = moe_exchange(rows, gate_pair, up_pair, down_pair).reshape(n_rows, model_dim)
        summed = base + dot32(spread, returned)
        return summed.astype(jnp.bfloat16).reshape(n_batch, seq_len, model_dim)

    return jax.shard_map(local_step, mesh=mesh, in_specs=(tok_spec, row_spec, row_spec, P("ep", "fsdp", None), P("ep", "fsdp", None), P("ep", None, "fsdp"), row_spec, row_spec, P(None, "fsdp"), tok_spec, tok_spec, tok_spec), out_specs=tok_spec, check_vma=False)
```

```python
import functools

import jax
import jax.numpy as jnp
from jax import lax
from jax.experimental import pallas as pl
from jax.experimental.pallas import tpu as pltpu
from jax.sharding import PartitionSpec as P

HEAD_DIM = 128
ROPE_BASE = 10000.0
EPSILON = 1e-6
RING = 4
BLOCK = 8
TURNS = 3
WIDE = 256
MESH = pl.DeviceIdType.MESH
STRIDES = (RING * RING, RING, 1)


def rms_norm(values):
    vals_f32 = values.astype(jnp.float32)
    mean_sq = jnp.mean(vals_f32 * vals_f32, axis=-1, keepdims=True)
    return (vals_f32 * lax.rsqrt(mean_sq + EPSILON)).astype(jnp.bfloat16)


def rotary_embed(heads_in, positions):
    half_dim = HEAD_DIM // 2
    inv_freq = ROPE_BASE ** (-jnp.arange(half_dim, dtype=jnp.float32) * (2.0 / HEAD_DIM))
    angles = positions[:, None] * inv_freq[None, :]
    cos_tab = jnp.cos(angles)[:, None, :]
    sin_tab = jnp.sin(angles)[:, None, :]
    vals_f32 = heads_in.astype(jnp.float32)
    first_half = vals_f32[..., :half_dim]
    second_half = vals_f32[..., half_dim:]
    rotated = jnp.concatenate([first_half * cos_tab - second_half * sin_tab, second_half * cos_tab + first_half * sin_tab], axis=-1)
    return rotated.astype(jnp.bfloat16)


def dot32(left, right):
    return jnp.dot(left, right, preferred_element_type=jnp.float32)


def split_cols(values, fs):
    half = values.shape[-1] // 2
    own = lax.dynamic_slice_in_dim(values, fs * half, half, axis=values.ndim - 1)
    other = lax.dynamic_slice_in_dim(values, (1 - fs) * half, half, axis=values.ndim - 1)
    return own, other


def paired_dot(own_other, pair):
    return dot32(own_other[0], pair[0]) + dot32(own_other[1], pair[1])


def attention_block(x_in, qkv_pair, out_pair, fs):
    n_batch, seq_len, model_dim = x_in.shape
    n_heads = qkv_pair[0].shape[1] // (3 * HEAD_DIM)
    normed = rms_norm(x_in).reshape(n_batch * seq_len, model_dim)
    qkv_proj = paired_dot(split_cols(normed, fs), qkv_pair).astype(jnp.bfloat16)
    qkv_proj = qkv_proj.reshape(n_batch, seq_len, 3, n_heads, HEAD_DIM)
    positions = jnp.arange(seq_len, dtype=jnp.float32)
    query_rot = rotary_embed(qkv_proj[:, :, 0], positions)
    key_rot = rotary_embed(qkv_proj[:, :, 1], positions)
    scores = jnp.einsum("bqhd,bkhd->bhqk", query_rot, key_rot, preferred_element_type=jnp.float32) * (HEAD_DIM ** -0.5)
    causal = jnp.arange(seq_len)[:, None] >= jnp.arange(seq_len)[None, :]
    attn_probs = jax.nn.softmax(jnp.where(causal, scores, -1e30), axis=-1).astype(jnp.bfloat16)
    attn_mixed = jnp.einsum("bhqk,bkhd->bqhd", attn_probs, qkv_proj[:, :, 2], preferred_element_type=jnp.float32).astype(jnp.bfloat16)
    mixed = split_cols(attn_mixed.reshape(n_batch * seq_len, n_heads * HEAD_DIM), fs)
    return (x_in.reshape(n_batch * seq_len, model_dim).astype(jnp.float32) + paired_dot(mixed, out_pair)).astype(jnp.bfloat16)


def capacity_for(n_tokens, top_k, n_experts):
    return ((5 * n_tokens * top_k) // (4 * n_experts) + 7) // 8 * 8


def ring_peer(me, axis, offset):
    stride = STRIDES[axis]
    place = lax.rem(me // stride, RING)
    return me + (lax.rem(place + offset + RING, RING) - place) * stride


class Exchange:
    def __init__(self, me, axes, sign, first, second, third, last, send, recv):
        self.me, self.axes, self.sign = me, axes, sign
        self.first, self.second, self.third, self.last = first, second, third, last
        self.send, self.recv = send, recv

    def push(self, phase, step, pairs):
        peer = ring_peer(self.me, self.axes[phase], self.sign * step)
        for src, dst in pairs:
            pltpu.make_async_remote_copy(src_ref=src, dst_ref=dst, send_sem=self.send.at[phase], recv_sem=self.recv.at[phase],
                                         device_id={"ep": peer}, device_id_type=MESH).start()

    def start(self, phase):
        for d in (1, 3, 2):
            if phase == 0:
                pairs = [(self.first.at[d], self.second.at[:, :, d - 1])]
            elif phase == 1:
                pairs = [(self.first.at[0, d], self.third.at[:, d - 1, 0]), (self.second.at[d], self.third.at[:, d - 1, pl.ds(1, 3)])]
            else:
                pairs = [(self.first.at[0, 0, d], self.last.at[d - 1, 0, 0]), (self.second.at[0, d], self.last.at[d - 1, 0, pl.ds(1, 3)]),
                         (self.third.at[d], self.last.at[d - 1, pl.ds(1, 3)])]
            self.push(phase, d, pairs)

    def landing(self, phase):
        return (self.second, self.third, self.last)[phase]

    def wait_recv(self, phase):
        whole = self.landing(phase)
        pltpu.make_async_copy(whole, whole, self.recv.at[phase]).wait()

    def wait_send(self, phase):
        whole = self.landing(phase)
        pltpu.make_async_copy(whole, whole, self.send.at[phase]).wait()

    def kept(self):
        return [(self.third.at[0], (0, pl.ds(1, 3))), (self.second.at[0, 0], (0, 0, pl.ds(1, 3))), (self.first.at[0, 0, 0], (0, 0, 0))]


def moe_kernel(n_units, top_k, rows_hbm, normed_ref, hidden_ref, place_ref, weight_ref,
               gate_a, gate_b, up_a, up_b, down_a, down_b, sgate_a, sgate_b, sup_a, sup_b, sdown_a, sdown_b, sum_ref,
               out1, out2, out3, made_hbm, back1, back2, back3,
               ga, gb, ua, ub, da, db, sin_ref, sdn_ref, x_ref, act_ref, y_ref, total_ref, mix_ref,
               w_sem, s_sem, x_sem, y_sem, go_send, go_recv, come_send, come_recv):
    me = lax.axis_index("ep")
    fs = lax.axis_index("fsdp")
    barrier = pltpu.get_barrier_semaphore()
    for axis in range(3):
        for d in range(1, RING):
            pl.semaphore_signal(barrier, inc=1, device_id={"ep": ring_peer(me, axis, d)}, device_id_type=MESH)
    pl.semaphore_wait(barrier, 3 * (RING - 1))

    half = ga.shape[0]
    inner = ga.shape[1]
    rows = RING ** 3 * BLOCK
    n_tokens = normed_ref.shape[0]
    go, come = [], []
    for u in range(n_units):
        axes = tuple((u % TURNS + k) % 3 for k in range(3))
        go.append(Exchange(me, axes, 1, rows_hbm.at[u], out1.at[u], out2.at[u], out3.at[u], go_send.at[u], go_recv.at[u]))
        come.append(Exchange(me, axes[::-1], -1, made_hbm.at[u], back1.at[u], back2.at[u], back3.at[u], come_send.at[u], come_recv.at[u]))
    units = range(n_units)
    first, second = range(TURNS), range(TURNS, n_units)

    def own(side):
        return pl.ds(pl.multiple_of(lax.rem(fs + side, 2) * half, half), half)

    def own_block(side, n):
        return pl.ds(pl.multiple_of(lax.rem(fs + side, 2) * half + n * WIDE, WIDE), WIDE)

    def block_at(n):
        return pl.ds(pl.multiple_of(n * WIDE, WIDE), WIDE)

    def shared_copies(n, slot):
        pairs = [(src.at[:, block_at(n)], sin_ref.at[slot, k]) for k, src in enumerate((sgate_a, sgate_b, sup_a, sup_b))]
        pairs += [(src.at[block_at(n)], sdn_ref.at[slot, k]) for k, src in enumerate((sdown_a, sdown_b))]
        return [pltpu.make_async_copy(src, dst, s_sem.at[slot, k]) for k, (src, dst) in enumerate(pairs)]

    for copy in shared_copies(0, 0):
        copy.start()
    for u in units:
        go[u].start(0)
    weights = [pltpu.make_async_copy(src, dst, w_sem.at[n]) for n, (src, dst) in enumerate(
        ((gate_a, ga), (gate_b, gb), (up_a, ua), (up_b, ub), (down_a, da), (down_b, db)))]
    for copy in weights:
        copy.start()
    total_ref[...] = hidden_ref[...].astype(jnp.float32)

    n_shared = sgate_a.shape[1] // WIDE

    def shared_step(n, carry):
        slot = lax.rem(n, 2)
        for copy in shared_copies(n, slot):
            copy.wait()

        @pl.when(n + 1 < n_shared)
        def _():
            for copy in shared_copies(n + 1, 1 - slot):
                copy.start()

        left, right = normed_ref[:, own(0)], normed_ref[:, own(1)]
        gate = dot32(left, sin_ref[slot, 0]) + dot32(right, sin_ref[slot, 1])
        up = dot32(left, sin_ref[slot, 2]) + dot32(right, sin_ref[slot, 3])
        act_ref[pl.ds(0, n_tokens), pl.ds(0, WIDE)] = (jax.nn.silu(gate) * up).astype(jnp.bfloat16)

        def shared_down(m, c):
            for side in range(2):
                total_ref[:, own_block(side, m)] += dot32(act_ref[pl.ds(0, n_tokens), pl.ds(0, WIDE)], sdn_ref[slot, side, :, block_at(m)])
            return c

        lax.fori_loop(0, half // WIDE, shared_down, 0)
        return carry

    lax.fori_loop(0, n_shared, shared_step, 0)

    def advance(exchange, phase):
        exchange.wait_recv(phase)
        exchange.start(phase + 1)

    for phase in range(2):
        for u in units:
            advance(go[u], phase)
    for copy in weights:
        copy.wait()

    def loads(exchange, slot):
        pieces = [(exchange.last, (pl.ds(1, 3),))] + exchange.kept()
        return [pltpu.make_async_copy(src, x_ref.at[(slot, *place)], x_sem.at[slot, n]) for n, (src, place) in enumerate(pieces)]

    def fetch(exchange, slot):
        exchange.wait_recv(2)
        for copy in loads(exchange, slot):
            copy.start()

    def expert(slot):
        x2 = x_ref.at[slot].reshape(rows, 2 * half)
        y2 = y_ref.at[slot].reshape(rows, 2 * half)

        def inner_block(cols):
            gate = dot32(x2[:, own(0)], ga[:, cols]) + dot32(x2[:, own(1)], gb[:, cols])
            up = dot32(x2[:, own(0)], ua[:, cols]) + dot32(x2[:, own(1)], ub[:, cols])
            act_ref[:, cols] = (jax.nn.silu(gate) * up).astype(jnp.bfloat16)

        def inner_step(n, carry):
            inner_block(block_at(n))
            return carry

        whole = inner // WIDE
        lax.fori_loop(0, whole, inner_step, 0)
        if inner % WIDE:
            inner_block(pl.ds(whole * WIDE, inner % WIDE))

        def down_step(n, carry):
            for side, weight in enumerate((da, db)):
                y2[:, own_block(side, n)] = dot32(act_ref[...], weight[:, block_at(n)]).astype(jnp.bfloat16)
            return carry

        lax.fori_loop(0, half // WIDE, down_step, 0)

    fetch(go[0], 0)
    for u in units:
        slot = u % 2
        for copy in loads(go[u], slot):
            copy.wait()
        if u + 1 < n_units:
            fetch(go[u + 1], 1 - slot)
        expert(slot)
        copy = pltpu.make_async_copy(y_ref.at[slot], made_hbm.at[u], y_sem.at[slot])
        copy.start()
        copy.wait()
        come[u].start(0)
        if u == n_units - 3:
            advance(come[0], 0)
        if u == n_units - 2:
            advance(come[1], 0)
            advance(come[2], 0)
    for u in second:
        advance(come[u], 0)
    for u in units:
        advance(come[u], 1)

    def mix(u, slot):
        for c in range(rows // 128):
            at = lax.broadcasted_iota(jnp.int32, (n_tokens, 128), 1) + (u * rows + c * 128)
            part = jnp.zeros((n_tokens, 128), jnp.float32)
            for k in range(top_k):
                part += jnp.where(place_ref[:, k:k + 1] == at, weight_ref[:, k:k + 1], 0.0)
            mix_ref[:, c * 128:(c + 1) * 128] = part.astype(jnp.bfloat16)
        for copy in loads(come[u], slot):
            copy.wait()
        if u + 1 < n_units:
            fetch(come[u + 1], 1 - slot)
        x2 = x_ref.at[slot].reshape(rows, 2 * half)

        def mix_step(n, carry):
            total_ref[:, block_at(n)] += dot32(mix_ref[...], x2[:, block_at(n)])
            return carry

        lax.fori_loop(0, 2 * half // WIDE, mix_step, 0)

    fetch(come[0], 0)
    for u in units:
        mix(u, u % 2)
    sum_ref[...] = total_ref[...].astype(jnp.bfloat16)
    for u in units:
        for phase in range(3):
            go[u].wait_send(phase)
            come[u].wait_send(phase)


def moe_exchange(rows, normed, hidden, place, weight, gate_pair, up_pair, down_pair, sgate_pair, sup_pair, sdown_pair):
    n_units, width = rows.shape[0], rows.shape[-1]
    n_tokens = normed.shape[0]
    anywhere = pl.BlockSpec(memory_space=pl.ANY)
    vmem = pl.BlockSpec(memory_space=pltpu.VMEM)
    weights = (*gate_pair, *up_pair, *down_pair)
    shared = (*sgate_pair, *sup_pair, *sdown_pair)
    inner = gate_pair[0].shape[1]

    def blocks(*lead):
        return jax.ShapeDtypeStruct((n_units, *lead, BLOCK, width), jnp.bfloat16)

    cube = (RING, RING, RING, BLOCK, width)
    steps = [blocks(4, 4, 3), blocks(4, 3, 4), blocks(3, 4, 4)]
    outs = [jax.ShapeDtypeStruct((n_tokens, width), jnp.bfloat16)] + steps + [blocks(4, 4, 4)] + steps
    sems = pltpu.SemaphoreType.DMA
    return pl.pallas_call(
        functools.partial(moe_kernel, n_units, place.shape[1]),
        out_shape=tuple(outs),
        in_specs=[anywhere] + [vmem] * 4 + [anywhere] * 12,
        out_specs=(vmem,) + (anywhere,) * 7,
        scratch_shapes=[pltpu.VMEM(w.shape, jnp.bfloat16) for w in weights] + [
            pltpu.VMEM((2, 4, width // 2, WIDE), jnp.bfloat16),
            pltpu.VMEM((2, 2, WIDE, width // 2), jnp.bfloat16),
            pltpu.VMEM((2, *cube), jnp.bfloat16),
            pltpu.VMEM((RING ** 3 * BLOCK, inner), jnp.bfloat16),
            pltpu.VMEM((2, *cube), jnp.bfloat16),
            pltpu.VMEM((n_tokens, width), jnp.float32),
            pltpu.VMEM((n_tokens, RING ** 3 * BLOCK), jnp.bfloat16),
            sems((6,)), sems((2, 6)), sems((2, 4)), sems((2,)),
            sems((n_units, 3)), sems((n_units, 3)), sems((n_units, 3)), sems((n_units, 3)),
        ],
        compiler_params=pltpu.CompilerParams(collective_id=0, has_side_effects=True, vmem_limit_bytes=60 * 1024 * 1024),
        cost_estimate=pl.CostEstimate(flops=250_000_000_000, bytes_accessed=100_000_000, transcendentals=0),
        name="moe_exchange",
    )(rows, normed, hidden, place, weight, *weights, *shared)[0]


def solution(mesh):
    n_ep = mesh.shape["ep"]
    tok_spec = P(("data", "fsdp", "ep"))
    row_spec = P("fsdp", None)

    def local_step(x_in, w_qkv, w_out, w_gate, w_up, w_down, ws_gate, ws_up, ws_down, expert_ids, slot_ids, gate_vals):
        n_batch, seq_len, model_dim = x_in.shape
        n_tokens = n_batch * seq_len
        top_k = expert_ids.shape[-1]
        n_experts = w_gate.shape[0] * n_ep
        capacity = capacity_for(n_tokens, top_k, n_experts)
        n_rows = n_experts * capacity
        fs = lax.axis_index("fsdp")

        def paired(weight):
            return weight, lax.ppermute(weight, "fsdp", [(0, 1), (1, 0)])

        qkv_pair, out_pair = paired(w_qkv), paired(w_out)
        gate_pair, up_pair, down_pair = paired(w_gate[0]), paired(w_up[0]), paired(w_down[0])
        sgate_pair, sup_pair, sdown_pair = paired(ws_gate), paired(ws_up), paired(ws_down)

        ids_flat = expert_ids.reshape(n_tokens, top_k)
        slots_flat = slot_ids.reshape(n_tokens, top_k)
        me = lax.axis_index("ep")
        rel = [lax.rem(ids_flat // s - me // s + n_ep, RING) for s in STRIDES]
        unit, within = slots_flat // BLOCK, slots_flat % BLOCK
        turn = unit % TURNS
        place = jnp.zeros_like(slots_flat)
        for r in range(TURNS):
            order = [rel[(r + k) % 3] for k in range(3)]
            place = jnp.where(turn == r, (order[0] * RING + order[1]) * RING + order[2], place)
        row_of = jnp.where(slots_flat >= 0, (unit * n_experts + place) * BLOCK + within, -1)
        row_iota = jnp.arange(n_rows, dtype=jnp.int32)
        gates = gate_vals.reshape(n_tokens, top_k)
        picks = sum((row_iota[:, None] == row_of[None, :, k]).astype(jnp.bfloat16) for k in range(top_k))

        hidden = attention_block(x_in, qkv_pair, out_pair, fs)
        normed = rms_norm(hidden)
        buffer = dot32(picks, normed).astype(jnp.bfloat16)
        rows = buffer.reshape(capacity // BLOCK, RING, RING, RING, BLOCK, model_dim)

        summed = moe_exchange(rows, normed, hidden, row_of, gates.astype(jnp.float32), gate_pair, up_pair, down_pair, sgate_pair, sup_pair, sdown_pair)
        return summed.reshape(n_batch, seq_len, model_dim)

    return jax.shard_map(local_step, mesh=mesh, in_specs=(tok_spec, row_spec, row_spec, P("ep", "fsdp", None), P("ep", "fsdp", None), P("ep", None, "fsdp"), row_spec, row_spec, P(None, "fsdp"), tok_spec, tok_spec, tok_spec), out_specs=tok_spec, check_vma=False)
```

```python
import functools

import jax
import jax.numpy as jnp
import numpy as np
from jax import lax
from jax.experimental import pallas as pl
from jax.experimental.pallas import tpu as pltpu
from jax.sharding import PartitionSpec as P

HEAD_DIM = 128
ROPE_BASE = 10000.0
EPSILON = 1e-6
RING = 4
BLOCK = 8
TURNS = 3
WIDE = 256
MESH = pl.DeviceIdType.MESH
STRIDES = (RING * RING, RING, 1)


def rms_norm(values):
    vals_f32 = values.astype(jnp.float32)
    mean_sq = jnp.mean(vals_f32 * vals_f32, axis=-1, keepdims=True)
    return (vals_f32 * lax.rsqrt(mean_sq + EPSILON)).astype(jnp.bfloat16)


def rotary_tables(seq_len):
    half_dim = HEAD_DIM // 2
    inv_freq = (ROPE_BASE ** (-np.arange(half_dim) * (2.0 / HEAD_DIM))).astype(np.float32)
    angles = (np.arange(seq_len, dtype=np.float32)[:, None] * inv_freq[None, :]).astype(np.float64)
    cos_tab, sin_tab = np.cos(angles), np.sin(angles)
    return (np.concatenate([cos_tab, cos_tab], axis=1).astype(np.float32), np.concatenate([-sin_tab, sin_tab], axis=1).astype(np.float32))


def dot32(left, right):
    return jnp.dot(left, right, preferred_element_type=jnp.float32)


def norm_rows(src_ref, dst_ref, group=48):
    def step(g, carry):
        at = pl.ds(pl.multiple_of(g * group, group), group)
        dst_ref[at, :] = rms_norm(src_ref[at, :])
        return carry

    lax.fori_loop(0, src_ref.shape[0] // group, step, 0)


def attention_kernel(x_ref, cos_ref, sin_ref, qkv_hbm, out_hbm, hidden_ref, normed_ref,
                     a_ref, o_ref, own_ref, far_ref, wo_own, wo_far, own_sem, send_sem, recv_sem, wo_sem):
    fs = lax.axis_index("fsdp")
    partner = {"fsdp": 1 - fs}
    seq_len, width = x_ref.shape
    half = width // 2
    n_chunks = width // WIDE
    barrier = pltpu.get_barrier_semaphore()
    pl.semaphore_signal(barrier, inc=1, device_id=partner, device_id_type=MESH)
    pl.semaphore_wait(barrier, 1)
    for c in range(n_chunks):
        for t in range(3):
            cols = qkv_hbm.at[:, pl.ds(t * width + c * WIDE, WIDE)]
            pltpu.make_async_remote_copy(src_ref=cols, dst_ref=far_ref.at[c, t], send_sem=send_sem.at[c], recv_sem=recv_sem.at[c],
                                         device_id=partner, device_id_type=MESH).start()
            pltpu.make_async_copy(cols, own_ref.at[c, t], own_sem.at[c]).start()
    wo_push = pltpu.make_async_remote_copy(src_ref=out_hbm, dst_ref=wo_far, send_sem=send_sem.at[n_chunks], recv_sem=recv_sem.at[n_chunks],
                                           device_id=partner, device_id_type=MESH)
    wo_push.start()
    wo_load = pltpu.make_async_copy(out_hbm, wo_own, wo_sem)
    wo_load.start()
    norm_rows(x_ref, a_ref)

    def own(side):
        return pl.ds(pl.multiple_of(lax.rem(fs + side, 2) * half, half), half)

    def chunk_step(c, carry):
        pltpu.make_async_copy(own_ref.at[c], own_ref.at[c], own_sem.at[c]).wait()
        pltpu.make_async_copy(far_ref.at[c], far_ref.at[c], recv_sem.at[c]).wait()
        left, right = a_ref[:, own(0)], a_ref[:, own(1)]
        q, k, v = [(dot32(left, own_ref[c, t]) + dot32(right, far_ref[c, t])).astype(jnp.bfloat16) for t in range(3)]

        def rotate(vals):
            wide = vals.astype(jnp.float32)
            return (wide * cos_ref[...] + pltpu.roll(wide, HEAD_DIM // 2, 1) * sin_ref[...]).astype(jnp.bfloat16)

        heads = []
        for j in range(WIDE // HEAD_DIM):
            cols = slice(j * HEAD_DIM, (j + 1) * HEAD_DIM)
            query, key, value = rotate(q[:, cols]), rotate(k[:, cols]), v[:, cols]
            parts = []
            for i in range(seq_len // 128):
                span = (i + 1) * 128
                scores = lax.dot_general(query[i * 128:span], key[:span], (((1,), (1,)), ((), ())), preferred_element_type=jnp.float32) * (HEAD_DIM ** -0.5)
                row_at = lax.broadcasted_iota(jnp.int32, (128, span), 0) + i * 128
                col_at = lax.broadcasted_iota(jnp.int32, (128, span), 1)
                scores = jnp.where(row_at >= col_at, scores, -1e30)
                power = jnp.exp(scores - jnp.max(scores, axis=-1, keepdims=True))
                probs = (power / jnp.sum(power, axis=-1, keepdims=True)).astype(jnp.bfloat16)
                parts.append(dot32(probs, value[:span]).astype(jnp.bfloat16))
            heads.append(jnp.concatenate(parts, axis=0))
        o_ref[:, pl.ds(pl.multiple_of(c * WIDE, WIDE), WIDE)] = jnp.concatenate(heads, axis=1)
        return carry

    lax.fori_loop(0, n_chunks, chunk_step, 0)
    wo_load.wait()
    wo_push.wait_recv()

    def out_step(n, carry):
        cols = pl.ds(pl.multiple_of(n * WIDE, WIDE), WIDE)
        mixed = dot32(o_ref[:, own(0)], wo_own[:, cols]) + dot32(o_ref[:, own(1)], wo_far[:, cols])
        hidden_ref[:, cols] = (x_ref[:, cols].astype(jnp.float32) + mixed).astype(jnp.bfloat16)
        return carry

    lax.fori_loop(0, n_chunks, out_step, 0)
    norm_rows(hidden_ref, normed_ref)
    for c in range(n_chunks):
        pltpu.make_async_copy(far_ref.at[c], far_ref.at[c], send_sem.at[c]).wait()
    wo_push.wait_send()


def attention(x_rows, w_qkv, w_out):
    seq_len, width = x_rows.shape
    half, n_chunks = width // 2, width // WIDE
    anywhere = pl.BlockSpec(memory_space=pl.ANY)
    vmem = pl.BlockSpec(memory_space=pltpu.VMEM)
    rows = jax.ShapeDtypeStruct((seq_len, width), jnp.bfloat16)
    sems = pltpu.SemaphoreType.DMA
    cos_tab, sin_tab = rotary_tables(seq_len)
    return pl.pallas_call(
        attention_kernel,
        out_shape=(rows, rows),
        in_specs=[vmem] * 3 + [anywhere] * 2,
        out_specs=(vmem, vmem),
        scratch_shapes=[
            pltpu.VMEM((seq_len, width), jnp.bfloat16),
            pltpu.VMEM((seq_len, width), jnp.bfloat16),
            pltpu.VMEM((n_chunks, 3, half, WIDE), jnp.bfloat16),
            pltpu.VMEM((n_chunks, 3, half, WIDE), jnp.bfloat16),
            pltpu.VMEM(w_out.shape, jnp.bfloat16),
            pltpu.VMEM(w_out.shape, jnp.bfloat16),
            sems((n_chunks,)), sems((n_chunks + 1,)), sems((n_chunks + 1,)), sems(()),
        ],
        compiler_params=pltpu.CompilerParams(collective_id=1, has_side_effects=True, vmem_limit_bytes=56 * 1024 * 1024),
        cost_estimate=pl.CostEstimate(flops=20_000_000_000, bytes_accessed=40_000_000, transcendentals=3_000_000),
        name="attention",
    )(x_rows, jnp.asarray(cos_tab), jnp.asarray(sin_tab), w_qkv, w_out)


def capacity_for(n_tokens, top_k, n_experts):
    return ((5 * n_tokens * top_k) // (4 * n_experts) + 7) // 8 * 8


def ring_peer(me, axis, offset):
    stride = STRIDES[axis]
    place = lax.rem(me // stride, RING)
    return me + (lax.rem(place + offset + RING, RING) - place) * stride


class Exchange:
    def __init__(self, me, axes, sign, first, second, third, last, send, recv):
        self.me, self.axes, self.sign = me, axes, sign
        self.first, self.second, self.third, self.last = first, second, third, last
        self.send, self.recv = send, recv

    def push(self, phase, step, pairs):
        peer = ring_peer(self.me, self.axes[phase], self.sign * step)
        for src, dst in pairs:
            pltpu.make_async_remote_copy(src_ref=src, dst_ref=dst, send_sem=self.send.at[phase], recv_sem=self.recv.at[phase],
                                         device_id={"ep": peer}, device_id_type=MESH).start()

    def start(self, phase):
        for d in (1, 3, 2):
            if phase == 0:
                pairs = [(self.first.at[d], self.second.at[:, :, d - 1])]
            elif phase == 1:
                pairs = [(self.first.at[0, d], self.third.at[:, d - 1, 0]), (self.second.at[d], self.third.at[:, d - 1, pl.ds(1, 3)])]
            else:
                pairs = [(self.first.at[0, 0, d], self.last.at[d - 1, 0, 0]), (self.second.at[0, d], self.last.at[d - 1, 0, pl.ds(1, 3)]),
                         (self.third.at[d], self.last.at[d - 1, pl.ds(1, 3)])]
            self.push(phase, d, pairs)

    def landing(self, phase):
        return (self.second, self.third, self.last)[phase]

    def wait_recv(self, phase):
        whole = self.landing(phase)
        pltpu.make_async_copy(whole, whole, self.recv.at[phase]).wait()

    def wait_send(self, phase):
        whole = self.landing(phase)
        pltpu.make_async_copy(whole, whole, self.send.at[phase]).wait()

    def kept(self):
        return [(self.third.at[0], (0, pl.ds(1, 3))), (self.second.at[0, 0], (0, 0, pl.ds(1, 3))), (self.first.at[0, 0, 0], (0, 0, 0))]


def moe_kernel(n_units, top_k, rows_hbm, normed_ref, hidden_ref, place_ref, weight_ref,
               gate_a, up_a, down_a, sgate_a, sup_a, sdown_a, sum_ref,
               sgate_b, sup_b, sdown_b, out1, out2, out3, made_hbm, back1, back2, back3,
               ga, gb, ua, ub, da, db, sin_ref, sdn_ref, x_ref, act_ref, y_ref, total_ref, mix_ref,
               w_sem, pair_send, pair_recv, far_send, far_recv, s_sem, x_sem, y_sem, go_send, go_recv, come_send, come_recv):
    me = lax.axis_index("ep")
    fs = lax.axis_index("fsdp")
    barrier = pltpu.get_barrier_semaphore()
    for axis in range(3):
        for d in range(1, RING):
            pl.semaphore_signal(barrier, inc=1, device_id={"ep": ring_peer(me, axis, d)}, device_id_type=MESH)
    partner = {"fsdp": 1 - fs}
    pl.semaphore_signal(barrier, inc=1, device_id=partner, device_id_type=MESH)
    pl.semaphore_wait(barrier, 3 * (RING - 1) + 1)

    half = ga.shape[0]
    inner = ga.shape[1]
    rows = RING ** 3 * BLOCK
    n_tokens = normed_ref.shape[0]
    go, come = [], []
    for u in range(n_units):
        axes = tuple((u % TURNS + k) % 3 for k in range(3))
        go.append(Exchange(me, axes, 1, rows_hbm.at[u], out1.at[u], out2.at[u], out3.at[u], go_send.at[u], go_recv.at[u]))
        come.append(Exchange(me, axes[::-1], -1, made_hbm.at[u], back1.at[u], back2.at[u], back3.at[u], come_send.at[u], come_recv.at[u]))
    units = range(n_units)
    first, second = range(TURNS), range(TURNS, n_units)

    def own(side):
        return pl.ds(pl.multiple_of(lax.rem(fs + side, 2) * half, half), half)

    def own_block(side, n):
        return pl.ds(pl.multiple_of(lax.rem(fs + side, 2) * half + n * WIDE, WIDE), WIDE)

    def block_at(n):
        return pl.ds(pl.multiple_of(n * WIDE, WIDE), WIDE)

    def shared_copies(n, slot):
        pairs = [(src, sin_ref.at[slot, k]) for k, src in enumerate((sgate_a.at[:, block_at(n)], sgate_b.at[n], sup_a.at[:, block_at(n)], sup_b.at[n]))]
        pairs += [(src.at[block_at(n)], sdn_ref.at[slot, k]) for k, src in enumerate((sdown_a, sdown_b))]
        return [pltpu.make_async_copy(src, dst, s_sem.at[slot, k]) for k, (src, dst) in enumerate(pairs)]

    def shared_push(n):
        pairs = [(sgate_a.at[:, block_at(n)], sgate_b.at[n]), (sup_a.at[:, block_at(n)], sup_b.at[n]), (sdown_a.at[block_at(n)], sdown_b.at[block_at(n)])]
        return [pltpu.make_async_remote_copy(src_ref=src, dst_ref=dst, send_sem=pair_send.at[k, n], recv_sem=pair_recv.at[k, n],
                                             device_id=partner, device_id_type=MESH) for k, (src, dst) in enumerate(pairs)]

    n_shared = sgate_a.shape[1] // WIDE
    ahead = 3
    for n in range(ahead):
        for copy in shared_push(n):
            copy.start()
    for u in units:
        go[u].start(0)
    weights = [pltpu.make_async_copy(src, dst, w_sem.at[n]) for n, (src, dst) in enumerate(((gate_a, ga), (up_a, ua), (down_a, da)))]
    far_weights = [pltpu.make_async_remote_copy(src_ref=src, dst_ref=dst, send_sem=far_send.at[n], recv_sem=far_recv.at[n], device_id=partner, device_id_type=MESH)
                   for n, (src, dst) in enumerate(((gate_a, gb), (up_a, ub), (down_a, db)))]
    for copy in weights:
        copy.start()
    for copy in shared_push(0):
        copy.wait_recv()
    for copy in shared_copies(0, 0):
        copy.start()
    total_ref[...] = hidden_ref[...].astype(jnp.float32)

    def shared_step(n, carry):
        slot = lax.rem(n, 2)
        for copy in shared_copies(n, slot):
            copy.wait()

        @pl.when(n + ahead < n_shared)
        def _():
            for copy in shared_push(n + ahead):
                copy.start()

        @pl.when(n + 1 < n_shared)
        def _():
            for copy in shared_push(n + 1):
                copy.wait_recv()
            for copy in shared_copies(n + 1, 1 - slot):
                copy.start()

        left, right = normed_ref[:, own(0)], normed_ref[:, own(1)]
        gate = dot32(left, sin_ref[slot, 0]) + dot32(right, sin_ref[slot, 1])
        up = dot32(left, sin_ref[slot, 2]) + dot32(right, sin_ref[slot, 3])
        act_ref[pl.ds(0, n_tokens), pl.ds(0, WIDE)] = (jax.nn.silu(gate) * up).astype(jnp.bfloat16)

        def shared_down(m, c):
            for side in range(2):
                total_ref[:, own_block(side, m)] += dot32(act_ref[pl.ds(0, n_tokens), pl.ds(0, WIDE)], sdn_ref[slot, side, :, block_at(m)])
            return c

        lax.fori_loop(0, half // WIDE, shared_down, 0)
        return carry

    lax.fori_loop(0, n_shared, shared_step, 0)
    for copy in far_weights:
        copy.start()

    def advance(exchange, phase):
        exchange.wait_recv(phase)
        exchange.start(phase + 1)

    for phase in range(2):
        for u in units:
            advance(go[u], phase)
    for copy in weights:
        copy.wait()
    for copy in far_weights:
        copy.wait_recv()

    def loads(exchange, slot):
        pieces = [(exchange.last, (pl.ds(1, 3),))] + exchange.kept()
        return [pltpu.make_async_copy(src, x_ref.at[(slot, *place)], x_sem.at[slot, n]) for n, (src, place) in enumerate(pieces)]

    def fetch(exchange, slot):
        exchange.wait_recv(2)
        for copy in loads(exchange, slot):
            copy.start()

    def expert(slot):
        x2 = x_ref.at[slot].reshape(rows, 2 * half)
        y2 = y_ref.at[slot].reshape(rows, 2 * half)

        def inner_block(cols):
            gate = dot32(x2[:, own(0)], ga[:, cols]) + dot32(x2[:, own(1)], gb[:, cols])
            up = dot32(x2[:, own(0)], ua[:, cols]) + dot32(x2[:, own(1)], ub[:, cols])
            act_ref[:, cols] = (jax.nn.silu(gate) * up).astype(jnp.bfloat16)

        def inner_step(n, carry):
            inner_block(block_at(n))
            return carry

        whole = inner // WIDE
        lax.fori_loop(0, whole, inner_step, 0)
        if inner % WIDE:
            inner_block(pl.ds(whole * WIDE, inner % WIDE))

        def down_step(n, carry):
            for side, weight in enumerate((da, db)):
                y2[:, own_block(side, n)] = dot32(act_ref[...], weight[:, block_at(n)]).astype(jnp.bfloat16)
            return carry

        lax.fori_loop(0, half // WIDE, down_step, 0)

    fetch(go[0], 0)
    for u in units:
        slot = u % 2
        for copy in loads(go[u], slot):
            copy.wait()
        if u + 1 < n_units:
            fetch(go[u + 1], 1 - slot)
        expert(slot)
        copy = pltpu.make_async_copy(y_ref.at[slot], made_hbm.at[u], y_sem.at[slot])
        copy.start()
        copy.wait()
        come[u].start(0)
        if u == n_units - 3:
            advance(come[0], 0)
        if u == n_units - 2:
            advance(come[1], 0)
            advance(come[2], 0)
    for u in second:
        advance(come[u], 0)
    for u in units:
        advance(come[u], 1)

    def mix(u, slot):
        for c in range(rows // 128):
            at = lax.broadcasted_iota(jnp.int32, (n_tokens, 128), 1) + (u * rows + c * 128)
            part = jnp.zeros((n_tokens, 128), jnp.float32)
            for k in range(top_k):
                part += jnp.where(place_ref[:, k:k + 1] == at, weight_ref[:, k:k + 1], 0.0)
            mix_ref[:, c * 128:(c + 1) * 128] = part.astype(jnp.bfloat16)
        for copy in loads(come[u], slot):
            copy.wait()
        if u + 1 < n_units:
            fetch(come[u + 1], 1 - slot)
        x2 = x_ref.at[slot].reshape(rows, 2 * half)

        def mix_step(n, carry):
            total_ref[:, block_at(n)] += dot32(mix_ref[...], x2[:, block_at(n)])
            return carry

        lax.fori_loop(0, 2 * half // WIDE, mix_step, 0)

    fetch(come[0], 0)
    for u in units:
        mix(u, u % 2)
    sum_ref[...] = total_ref[...].astype(jnp.bfloat16)
    for copy in far_weights:
        copy.wait_send()

    def pair_done(n, carry):
        for copy in shared_push(n):
            copy.wait_send()
        return carry

    lax.fori_loop(0, n_shared, pair_done, 0)
    for u in units:
        for phase in range(3):
            go[u].wait_send(phase)
            come[u].wait_send(phase)


def moe_exchange(rows, normed, hidden, place, weight, weights, shared):
    n_units, width = rows.shape[0], rows.shape[-1]
    n_tokens = normed.shape[0]
    anywhere = pl.BlockSpec(memory_space=pl.ANY)
    vmem = pl.BlockSpec(memory_space=pltpu.VMEM)
    inner, n_shared = weights[0].shape[1], shared[0].shape[1] // WIDE

    def blocks(*lead):
        return jax.ShapeDtypeStruct((n_units, *lead, BLOCK, width), jnp.bfloat16)

    cube = (RING, RING, RING, BLOCK, width)
    steps = [blocks(4, 4, 3), blocks(4, 3, 4), blocks(3, 4, 4)]
    wide_block = jax.ShapeDtypeStruct((n_shared, width // 2, WIDE), jnp.bfloat16)
    far = [wide_block, wide_block, jax.ShapeDtypeStruct(shared[2].shape, jnp.bfloat16)]
    outs = [jax.ShapeDtypeStruct((n_tokens, width), jnp.bfloat16)] + far + steps + [blocks(4, 4, 4)] + steps
    sems = pltpu.SemaphoreType.DMA
    return pl.pallas_call(
        functools.partial(moe_kernel, n_units, place.shape[1]),
        out_shape=tuple(outs),
        in_specs=[anywhere] + [vmem] * 4 + [anywhere] * 6,
        out_specs=(vmem,) + (anywhere,) * 10,
        scratch_shapes=[pltpu.VMEM(w.shape, jnp.bfloat16) for w in weights for _ in range(2)] + [
            pltpu.VMEM((2, 4, width // 2, WIDE), jnp.bfloat16),
            pltpu.VMEM((2, 2, WIDE, width // 2), jnp.bfloat16),
            pltpu.VMEM((2, *cube), jnp.bfloat16),
            pltpu.VMEM((RING ** 3 * BLOCK, inner), jnp.bfloat16),
            pltpu.VMEM((2, *cube), jnp.bfloat16),
            pltpu.VMEM((n_tokens, width), jnp.float32),
            pltpu.VMEM((n_tokens, RING ** 3 * BLOCK), jnp.bfloat16),
            sems((3,)), sems((3, n_shared)), sems((3, n_shared)), sems((3,)), sems((3,)), sems((2, 6)), sems((2, 4)), sems((2,)),
            sems((n_units, 3)), sems((n_units, 3)), sems((n_units, 3)), sems((n_units, 3)),
        ],
        compiler_params=pltpu.CompilerParams(collective_id=0, has_side_effects=True, vmem_limit_bytes=60 * 1024 * 1024),
        cost_estimate=pl.CostEstimate(flops=250_000_000_000, bytes_accessed=100_000_000, transcendentals=0),
        name="moe_exchange",
    )(rows, normed, hidden, place, weight, *weights, *shared)[0]


def solution(mesh):
    n_ep = mesh.shape["ep"]
    tok_spec = P(("data", "fsdp", "ep"))
    row_spec = P("fsdp", None)

    def local_step(x_in, w_qkv, w_out, w_gate, w_up, w_down, ws_gate, ws_up, ws_down, expert_ids, slot_ids, gate_vals):
        n_batch, seq_len, model_dim = x_in.shape
        n_tokens = n_batch * seq_len
        top_k = expert_ids.shape[-1]
        n_experts = w_gate.shape[0] * n_ep
        capacity = capacity_for(n_tokens, top_k, n_experts)
        n_rows = n_experts * capacity
        ids_flat = expert_ids.reshape(n_tokens, top_k)
        slots_flat = slot_ids.reshape(n_tokens, top_k)
        me = lax.axis_index("ep")
        rel = [lax.rem(ids_flat // s - me // s + n_ep, RING) for s in STRIDES]
        unit, within = slots_flat // BLOCK, slots_flat % BLOCK
        turn = unit % TURNS
        place = jnp.zeros_like(slots_flat)
        for r in range(TURNS):
            order = [rel[(r + k) % 3] for k in range(3)]
            place = jnp.where(turn == r, (order[0] * RING + order[1]) * RING + order[2], place)
        row_of = jnp.where(slots_flat >= 0, (unit * n_experts + place) * BLOCK + within, -1)
        row_iota = jnp.arange(n_rows, dtype=jnp.int32)
        gates = gate_vals.reshape(n_tokens, top_k)
        picks = sum((row_iota[:, None] == row_of[None, :, k]).astype(jnp.bfloat16) for k in range(top_k))

        hidden, normed = attention(x_in.reshape(n_tokens, model_dim), w_qkv, w_out)
        buffer = dot32(picks, normed).astype(jnp.bfloat16)
        rows = buffer.reshape(capacity // BLOCK, RING, RING, RING, BLOCK, model_dim)

        summed = moe_exchange(rows, normed, hidden, row_of, gates.astype(jnp.float32), (w_gate[0], w_up[0], w_down[0]), (ws_gate, ws_up, ws_down))
        return summed.reshape(n_batch, seq_len, model_dim)

    return jax.shard_map(local_step, mesh=mesh, in_specs=(tok_spec, row_spec, row_spec, P("ep", "fsdp", None), P("ep", "fsdp", None), P("ep", None, "fsdp"), row_spec, row_spec, P(None, "fsdp"), tok_spec, tok_spec, tok_spec), out_specs=tok_spec, check_vma=False)
```

```python
import functools

import jax
import jax.numpy as jnp
import numpy as np
from jax import lax
from jax.experimental import pallas as pl
from jax.experimental.pallas import tpu as pltpu
from jax.sharding import PartitionSpec as P

HEAD_DIM = 128
ROPE_BASE = 10000.0
EPSILON = 1e-6
RING = 4
BLOCK = 8
TURNS = 3
WIDE = 256
MESH = pl.DeviceIdType.MESH
STRIDES = (RING * RING, RING, 1)


def rms_norm(values):
    vals_f32 = values.astype(jnp.float32)
    mean_sq = jnp.mean(vals_f32 * vals_f32, axis=-1, keepdims=True)
    return (vals_f32 * lax.rsqrt(mean_sq + EPSILON)).astype(jnp.bfloat16)


def rotary_tables(seq_len):
    half_dim = HEAD_DIM // 2
    inv_freq = (ROPE_BASE ** (-np.arange(half_dim) * (2.0 / HEAD_DIM))).astype(np.float32)
    angles = (np.arange(seq_len, dtype=np.float32)[:, None] * inv_freq[None, :]).astype(np.float64)
    cos_tab, sin_tab = np.cos(angles), np.sin(angles)
    return (np.concatenate([cos_tab, cos_tab], axis=1).astype(np.float32), np.concatenate([-sin_tab, sin_tab], axis=1).astype(np.float32))


def dot32(left, right):
    return jnp.dot(left, right, preferred_element_type=jnp.float32)


def norm_rows(src_ref, dst_ref, group=48):
    def step(g, carry):
        at = pl.ds(pl.multiple_of(g * group, group), group)
        dst_ref[at, :] = rms_norm(src_ref[at, :])
        return carry

    lax.fori_loop(0, src_ref.shape[0] // group, step, 0)


def attention_kernel(x_ref, cos_ref, sin_ref, qkv_hbm, out_hbm, hidden_ref, normed_ref,
                     a_ref, o_ref, own_ref, far_ref, wo_own, wo_far, own_sem, send_sem, recv_sem, wo_sem):
    fs = lax.axis_index("fsdp")
    partner = {"fsdp": 1 - fs}
    seq_len, width = x_ref.shape
    half = width // 2
    n_chunks = width // WIDE
    barrier = pltpu.get_barrier_semaphore()
    pl.semaphore_signal(barrier, inc=1, device_id=partner, device_id_type=MESH)
    pl.semaphore_wait(barrier, 1)
    for c in range(n_chunks):
        for t in range(3):
            cols = qkv_hbm.at[:, pl.ds(t * width + c * WIDE, WIDE)]
            pltpu.make_async_remote_copy(src_ref=cols, dst_ref=far_ref.at[c, t], send_sem=send_sem.at[c], recv_sem=recv_sem.at[c],
                                         device_id=partner, device_id_type=MESH).start()
            pltpu.make_async_copy(cols, own_ref.at[c, t], own_sem.at[c]).start()
    wo_push = pltpu.make_async_remote_copy(src_ref=out_hbm, dst_ref=wo_far, send_sem=send_sem.at[n_chunks], recv_sem=recv_sem.at[n_chunks],
                                           device_id=partner, device_id_type=MESH)
    wo_push.start()
    wo_load = pltpu.make_async_copy(out_hbm, wo_own, wo_sem)
    wo_load.start()
    norm_rows(x_ref, a_ref)

    def own(side):
        return pl.ds(pl.multiple_of(lax.rem(fs + side, 2) * half, half), half)

    def chunk_step(c, carry):
        pltpu.make_async_copy(own_ref.at[c], own_ref.at[c], own_sem.at[c]).wait()
        pltpu.make_async_copy(far_ref.at[c], far_ref.at[c], recv_sem.at[c]).wait()
        left, right = a_ref[:, own(0)], a_ref[:, own(1)]
        q, k, v = [(dot32(left, own_ref[c, t]) + dot32(right, far_ref[c, t])).astype(jnp.bfloat16) for t in range(3)]

        def rotate(vals):
            wide = vals.astype(jnp.float32)
            return (wide * cos_ref[...] + pltpu.roll(wide, HEAD_DIM // 2, 1) * sin_ref[...]).astype(jnp.bfloat16)

        heads = []
        for j in range(WIDE // HEAD_DIM):
            cols = slice(j * HEAD_DIM, (j + 1) * HEAD_DIM)
            query, key, value = rotate(q[:, cols]), rotate(k[:, cols]), v[:, cols]
            parts = []
            for i in range(seq_len // 128):
                span = (i + 1) * 128
                scores = lax.dot_general(query[i * 128:span], key[:span], (((1,), (1,)), ((), ())), preferred_element_type=jnp.float32) * (HEAD_DIM ** -0.5)
                row_at = lax.broadcasted_iota(jnp.int32, (128, span), 0) + i * 128
                col_at = lax.broadcasted_iota(jnp.int32, (128, span), 1)
                scores = jnp.where(row_at >= col_at, scores, -1e30)
                power = jnp.exp(scores - jnp.max(scores, axis=-1, keepdims=True))
                probs = (power / jnp.sum(power, axis=-1, keepdims=True)).astype(jnp.bfloat16)
                parts.append(dot32(probs, value[:span]).astype(jnp.bfloat16))
            heads.append(jnp.concatenate(parts, axis=0))
        o_ref[:, pl.ds(pl.multiple_of(c * WIDE, WIDE), WIDE)] = jnp.concatenate(heads, axis=1)
        return carry

    lax.fori_loop(0, n_chunks, chunk_step, 0)
    wo_load.wait()
    wo_push.wait_recv()

    def out_step(n, carry):
        cols = pl.ds(pl.multiple_of(n * WIDE, WIDE), WIDE)
        mixed = dot32(o_ref[:, own(0)], wo_own[:, cols]) + dot32(o_ref[:, own(1)], wo_far[:, cols])
        hidden_ref[:, cols] = (x_ref[:, cols].astype(jnp.float32) + mixed).astype(jnp.bfloat16)
        return carry

    lax.fori_loop(0, n_chunks, out_step, 0)
    norm_rows(hidden_ref, normed_ref)
    for c in range(n_chunks):
        pltpu.make_async_copy(far_ref.at[c], far_ref.at[c], send_sem.at[c]).wait()
    wo_push.wait_send()


def attention(x_rows, w_qkv, w_out):
    seq_len, width = x_rows.shape
    half, n_chunks = width // 2, width // WIDE
    anywhere = pl.BlockSpec(memory_space=pl.ANY)
    vmem = pl.BlockSpec(memory_space=pltpu.VMEM)
    rows = jax.ShapeDtypeStruct((seq_len, width), jnp.bfloat16)
    sems = pltpu.SemaphoreType.DMA
    cos_tab, sin_tab = rotary_tables(seq_len)
    return pl.pallas_call(
        attention_kernel,
        out_shape=(rows, rows),
        in_specs=[vmem] * 3 + [anywhere] * 2,
        out_specs=(vmem, vmem),
        scratch_shapes=[
            pltpu.VMEM((seq_len, width), jnp.bfloat16),
            pltpu.VMEM((seq_len, width), jnp.bfloat16),
            pltpu.VMEM((n_chunks, 3, half, WIDE), jnp.bfloat16),
            pltpu.VMEM((n_chunks, 3, half, WIDE), jnp.bfloat16),
            pltpu.VMEM(w_out.shape, jnp.bfloat16),
            pltpu.VMEM(w_out.shape, jnp.bfloat16),
            sems((n_chunks,)), sems((n_chunks + 1,)), sems((n_chunks + 1,)), sems(()),
        ],
        compiler_params=pltpu.CompilerParams(collective_id=1, has_side_effects=True, vmem_limit_bytes=56 * 1024 * 1024),
        cost_estimate=pl.CostEstimate(flops=20_000_000_000, bytes_accessed=40_000_000, transcendentals=3_000_000),
        name="attention",
    )(x_rows, jnp.asarray(cos_tab), jnp.asarray(sin_tab), w_qkv, w_out)


def capacity_for(n_tokens, top_k, n_experts):
    return ((5 * n_tokens * top_k) // (4 * n_experts) + 7) // 8 * 8


def ring_peer(me, axis, offset):
    stride = RING * RING - 12 * axis + 9 * (axis * (axis - 1) // 2)
    place = lax.rem(me // stride, RING)
    return me + (lax.rem(place + offset + RING, RING) - place) * stride


class Exchange:
    def __init__(self, me, axes, sign, unit, buffers, send, recv):
        self.me, self.axes, self.sign = me, axes, sign
        self.first, self.second, self.third, self.last = [ref.at[unit] for ref in buffers]
        self.send, self.recv = send.at[unit], recv.at[unit]

    def push(self, phase, step, pairs):
        peer = ring_peer(self.me, self.axes[phase], self.sign * step)
        for src, dst in pairs:
            pltpu.make_async_remote_copy(src_ref=src, dst_ref=dst, send_sem=self.send.at[phase], recv_sem=self.recv.at[phase],
                                         device_id={"ep": peer}, device_id_type=MESH).start()

    def start(self, phase):
        for d in (1, 3, 2):
            if phase == 0:
                pairs = [(self.first.at[d], self.second.at[:, :, d - 1])]
            elif phase == 1:
                pairs = [(self.first.at[0, d], self.third.at[:, d - 1, 0]), (self.second.at[d], self.third.at[:, d - 1, pl.ds(1, 3)])]
            else:
                pairs = [(self.first.at[0, 0, d], self.last.at[d - 1, 0, 0]), (self.second.at[0, d], self.last.at[d - 1, 0, pl.ds(1, 3)]),
                         (self.third.at[d], self.last.at[d - 1, pl.ds(1, 3)])]
            self.push(phase, d, pairs)

    def landing(self, phase):
        return (self.second, self.third, self.last)[phase]

    def wait_recv(self, phase):
        whole = self.landing(phase)
        pltpu.make_async_copy(whole, whole, self.recv.at[phase]).wait()

    def wait_send(self, phase):
        whole = self.landing(phase)
        pltpu.make_async_copy(whole, whole, self.send.at[phase]).wait()

    def kept(self):
        return [(self.third.at[0], (0, pl.ds(1, 3))), (self.second.at[0, 0], (0, 0, pl.ds(1, 3))), (self.first.at[0, 0, 0], (0, 0, 0))]


def moe_kernel(n_units, normed_ref, hidden_ref, place_ref, weight_ref,
               gate_a, up_a, down_a, sgate_a, sup_a, sdown_a, sum_ref,
               sgate_b, sup_b, sdown_b, rows_hbm, out1, out2, out3, made_hbm, back1, back2, back3,
               ga, gb, ua, ub, da, db, sin_ref, sdn_ref, x_ref, act_ref, y_ref, total_ref, mix_ref, pick_ref,
               w_sem, pair_send, pair_recv, far_send, far_recv, s_sem, x_sem, y_sem, go_send, go_recv, come_send, come_recv):
    me = lax.axis_index("ep")
    fs = lax.axis_index("fsdp")
    barrier = pltpu.get_barrier_semaphore()
    for axis in range(3):
        for d in range(1, RING):
            pl.semaphore_signal(barrier, inc=1, device_id={"ep": ring_peer(me, axis, d)}, device_id_type=MESH)
    partner = {"fsdp": 1 - fs}
    pl.semaphore_signal(barrier, inc=1, device_id=partner, device_id_type=MESH)
    pl.semaphore_wait(barrier, 3 * (RING - 1) + 1)

    half = ga.shape[0]
    inner = ga.shape[1]
    rows = RING ** 3 * BLOCK
    n_tokens = normed_ref.shape[0]
    top_k = place_ref.shape[0]

    def go(u):
        return Exchange(me, [lax.rem(u + k, 3) for k in range(3)], 1, u, (rows_hbm, out1, out2, out3), go_send, go_recv)

    def come(u):
        return Exchange(me, [lax.rem(u + 2 - k, 3) for k in range(3)], -1, u, (made_hbm, back1, back2, back3), come_send, come_recv)

    def advance(exchange, phase):
        exchange.wait_recv(phase)
        exchange.start(phase + 1)

    def each(low, high, step):
        def body(u, carry):
            step(u)
            return carry

        lax.fori_loop(low, high, body, 0)

    def own(side):
        return pl.ds(pl.multiple_of(lax.rem(fs + side, 2) * half, half), half)

    def own_block(side, n):
        return pl.ds(pl.multiple_of(lax.rem(fs + side, 2) * half + n * WIDE, WIDE), WIDE)

    def block_at(n):
        return pl.ds(pl.multiple_of(n * WIDE, WIDE), WIDE)

    def shared_copies(n, slot):
        pairs = [(src, sin_ref.at[slot, k]) for k, src in enumerate((sgate_a.at[:, block_at(n)], sgate_b.at[n], sup_a.at[:, block_at(n)], sup_b.at[n]))]
        pairs += [(src.at[block_at(n)], sdn_ref.at[slot, k]) for k, src in enumerate((sdown_a, sdown_b))]
        return [pltpu.make_async_copy(src, dst, s_sem.at[slot, k]) for k, (src, dst) in enumerate(pairs)]

    def shared_push(n):
        pairs = [(sgate_a.at[:, block_at(n)], sgate_b.at[n]), (sup_a.at[:, block_at(n)], sup_b.at[n]), (sdown_a.at[block_at(n)], sdown_b.at[block_at(n)])]
        return [pltpu.make_async_remote_copy(src_ref=src, dst_ref=dst, send_sem=pair_send.at[k, n], recv_sem=pair_recv.at[k, n],
                                             device_id=partner, device_id_type=MESH) for k, (src, dst) in enumerate(pairs)]

    n_shared = sgate_a.shape[1] // WIDE
    ahead = 3
    for n in range(ahead):
        for copy in shared_push(n):
            copy.start()

    def pick(u):
        slot = lax.rem(u, 2)
        for c in range(rows // 128):
            at = lax.broadcasted_iota(jnp.int32, (128, n_tokens), 0) + (u * rows + c * 128)
            part = jnp.zeros((128, n_tokens), jnp.float32)
            for k in range(top_k):
                part += jnp.where(place_ref[k:k + 1, :] == at, 1.0, 0.0)
            pick_ref[c * 128:(c + 1) * 128, :] = part.astype(jnp.bfloat16)
        x2 = x_ref.at[slot].reshape(rows, 2 * half)

        def pick_step(n, carry):
            x2[:, block_at(n)] = dot32(pick_ref[...], normed_ref[:, block_at(n)]).astype(jnp.bfloat16)
            return carry

        lax.fori_loop(0, 2 * half // WIDE, pick_step, 0)
        copy = pltpu.make_async_copy(x_ref.at[slot], rows_hbm.at[u], y_sem.at[slot])
        copy.start()
        copy.wait()
        go(u).start(0)

    each(0, n_units, pick)
    weights = [pltpu.make_async_copy(src, dst, w_sem.at[n]) for n, (src, dst) in enumerate(((gate_a, ga), (up_a, ua), (down_a, da)))]
    far_weights = [pltpu.make_async_remote_copy(src_ref=src, dst_ref=dst, send_sem=far_send.at[n], recv_sem=far_recv.at[n], device_id=partner, device_id_type=MESH)
                   for n, (src, dst) in enumerate(((gate_a, gb), (up_a, ub), (down_a, db)))]
    for copy in weights:
        copy.start()
    for copy in shared_push(0):
        copy.wait_recv()
    for copy in shared_copies(0, 0):
        copy.start()
    total_ref[...] = hidden_ref[...].astype(jnp.float32)

    def shared_step(n, carry):
        slot = lax.rem(n, 2)
        for copy in shared_copies(n, slot):
            copy.wait()

        @pl.when(n == 4)
        def _():
            each(0, TURNS, lambda u: advance(go(u), 0))

        @pl.when(n + ahead < n_shared)
        def _():
            for copy in shared_push(n + ahead):
                copy.start()

        @pl.when(n + 1 < n_shared)
        def _():
            for copy in shared_push(n + 1):
                copy.wait_recv()
            for copy in shared_copies(n + 1, 1 - slot):
                copy.start()

        left, right = normed_ref[:, own(0)], normed_ref[:, own(1)]
        gate = dot32(left, sin_ref[slot, 0]) + dot32(right, sin_ref[slot, 1])
        up = dot32(left, sin_ref[slot, 2]) + dot32(right, sin_ref[slot, 3])
        act_ref[pl.ds(0, n_tokens), pl.ds(0, WIDE)] = (jax.nn.silu(gate) * up).astype(jnp.bfloat16)

        def shared_down(m, c):
            for side in range(2):
                total_ref[:, own_block(side, m)] += dot32(act_ref[pl.ds(0, n_tokens), pl.ds(0, WIDE)], sdn_ref[slot, side, :, block_at(m)])
            return c

        lax.fori_loop(0, half // WIDE, shared_down, 0)
        return carry

    lax.fori_loop(0, n_shared, shared_step, 0)
    for copy in far_weights:
        copy.start()

    each(TURNS, n_units, lambda u: advance(go(u), 0))
    each(0, n_units, lambda u: advance(go(u), 1))
    for copy in weights:
        copy.wait()
    for copy in far_weights:
        copy.wait_recv()

    def loads(exchange, slot):
        pieces = [(exchange.last, (pl.ds(1, 3),))] + exchange.kept()
        return [pltpu.make_async_copy(src, x_ref.at[(slot, *place)], x_sem.at[slot, n]) for n, (src, place) in enumerate(pieces)]

    def fetch(exchange, slot):
        exchange.wait_recv(2)
        for copy in loads(exchange, slot):
            copy.start()

    def expert(slot):
        x2 = x_ref.at[slot].reshape(rows, 2 * half)
        y2 = y_ref.at[slot].reshape(rows, 2 * half)

        def inner_block(cols):
            gate = dot32(x2[:, own(0)], ga[:, cols]) + dot32(x2[:, own(1)], gb[:, cols])
            up = dot32(x2[:, own(0)], ua[:, cols]) + dot32(x2[:, own(1)], ub[:, cols])
            act_ref[:, cols] = (jax.nn.silu(gate) * up).astype(jnp.bfloat16)

        def inner_step(n, carry):
            inner_block(block_at(n))
            return carry

        whole = inner // WIDE
        lax.fori_loop(0, whole, inner_step, 0)
        if inner % WIDE:
            inner_block(pl.ds(whole * WIDE, inner % WIDE))

        def down_step(n, carry):
            for side, weight in enumerate((da, db)):
                y2[:, own_block(side, n)] = dot32(act_ref[...], weight[:, block_at(n)]).astype(jnp.bfloat16)
            return carry

        lax.fori_loop(0, half // WIDE, down_step, 0)

    fetch(go(0), 0)

    def expert_unit(u):
        slot = lax.rem(u, 2)
        for copy in loads(go(u), slot):
            copy.wait()

        @pl.when(u + 1 < n_units)
        def _():
            fetch(go(u + 1), 1 - slot)

        expert(slot)
        copy = pltpu.make_async_copy(y_ref.at[slot], made_hbm.at[u], y_sem.at[slot])
        copy.start()
        copy.wait()
        come(u).start(0)

        @pl.when(u >= TURNS)
        def _():
            advance(come(u - TURNS), 0)

    each(0, n_units, expert_unit)
    each(n_units - TURNS, n_units, lambda u: advance(come(u), 0))
    each(0, n_units, lambda u: advance(come(u), 1))
    fetch(come(0), 0)

    def mix(u):
        slot = lax.rem(u, 2)
        for c in range(rows // 128):
            at = lax.broadcasted_iota(jnp.int32, (128, n_tokens), 0) + (u * rows + c * 128)
            part = jnp.zeros((128, n_tokens), jnp.float32)
            for k in range(top_k):
                part += jnp.where(place_ref[k:k + 1, :] == at, weight_ref[k:k + 1, :], 0.0)
            mix_ref[:, c * 128:(c + 1) * 128] = part.T.astype(jnp.bfloat16)
        for copy in loads(come(u), slot):
            copy.wait()

        @pl.when(u + 1 < n_units)
        def _():
            fetch(come(u + 1), 1 - slot)

        x2 = x_ref.at[slot].reshape(rows, 2 * half)

        def mix_step(n, carry):
            total_ref[:, block_at(n)] += dot32(mix_ref[...], x2[:, block_at(n)])
            return carry

        lax.fori_loop(0, 2 * half // WIDE, mix_step, 0)

    each(0, n_units, mix)
    sum_ref[...] = total_ref[...].astype(jnp.bfloat16)
    for copy in far_weights:
        copy.wait_send()

    def pair_done(n, carry):
        for copy in shared_push(n):
            copy.wait_send()
        return carry

    lax.fori_loop(0, n_shared, pair_done, 0)

    def sent(u):
        for phase in range(3):
            go(u).wait_send(phase)
            come(u).wait_send(phase)

    each(0, n_units, sent)


def moe_exchange(n_units, normed, hidden, place, weight, weights, shared):
    n_tokens, width = normed.shape
    anywhere = pl.BlockSpec(memory_space=pl.ANY)
    vmem = pl.BlockSpec(memory_space=pltpu.VMEM)
    inner, n_shared = weights[0].shape[1], shared[0].shape[1] // WIDE

    def blocks(*lead):
        return jax.ShapeDtypeStruct((n_units, *lead, BLOCK, width), jnp.bfloat16)

    cube = (RING, RING, RING, BLOCK, width)
    steps = [blocks(4, 4, 3), blocks(4, 3, 4), blocks(3, 4, 4)]
    wide_block = jax.ShapeDtypeStruct((n_shared, width // 2, WIDE), jnp.bfloat16)
    far = [wide_block, wide_block, jax.ShapeDtypeStruct(shared[2].shape, jnp.bfloat16)]
    outs = [jax.ShapeDtypeStruct((n_tokens, width), jnp.bfloat16)] + far + [blocks(4, 4, 4)] + steps + [blocks(4, 4, 4)] + steps
    sems = pltpu.SemaphoreType.DMA
    return pl.pallas_call(
        functools.partial(moe_kernel, n_units),
        out_shape=tuple(outs),
        in_specs=[vmem] * 4 + [anywhere] * 6,
        out_specs=(vmem,) + (anywhere,) * 11,
        scratch_shapes=[pltpu.VMEM(w.shape, jnp.bfloat16) for w in weights for _ in range(2)] + [
            pltpu.VMEM((2, 4, width // 2, WIDE), jnp.bfloat16),
            pltpu.VMEM((2, 2, WIDE, width // 2), jnp.bfloat16),
            pltpu.VMEM((2, *cube), jnp.bfloat16),
            pltpu.VMEM((RING ** 3 * BLOCK, inner), jnp.bfloat16),
            pltpu.VMEM((2, *cube), jnp.bfloat16),
            pltpu.VMEM((n_tokens, width), jnp.float32),
            pltpu.VMEM((n_tokens, RING ** 3 * BLOCK), jnp.bfloat16),
            pltpu.VMEM((RING ** 3 * BLOCK, n_tokens), jnp.bfloat16),
            sems((3,)), sems((3, n_shared)), sems((3, n_shared)), sems((3,)), sems((3,)), sems((2, 6)), sems((2, 4)), sems((2,)),
            sems((n_units, 3)), sems((n_units, 3)), sems((n_units, 3)), sems((n_units, 3)),
        ],
        compiler_params=pltpu.CompilerParams(collective_id=0, has_side_effects=True, vmem_limit_bytes=60 * 1024 * 1024),
        cost_estimate=pl.CostEstimate(flops=250_000_000_000, bytes_accessed=100_000_000, transcendentals=0),
        name="moe_exchange",
    )(normed, hidden, place, weight, *weights, *shared)[0]


def solution(mesh):
    n_ep = mesh.shape["ep"]
    tok_spec = P(("data", "fsdp", "ep"))
    row_spec = P("fsdp", None)

    def local_step(x_in, w_qkv, w_out, w_gate, w_up, w_down, ws_gate, ws_up, ws_down, expert_ids, slot_ids, gate_vals):
        n_batch, seq_len, model_dim = x_in.shape
        n_tokens = n_batch * seq_len
        top_k = expert_ids.shape[-1]
        n_experts = w_gate.shape[0] * n_ep
        capacity = capacity_for(n_tokens, top_k, n_experts)
        ids_flat = expert_ids.reshape(n_tokens, top_k).T
        slots_flat = slot_ids.reshape(n_tokens, top_k).T
        me = lax.axis_index("ep")
        rel = [lax.rem(ids_flat // s - me // s + n_ep, RING) for s in STRIDES]
        unit, within = slots_flat // BLOCK, slots_flat % BLOCK
        turn = unit % TURNS
        place = jnp.zeros_like(slots_flat)
        for r in range(TURNS):
            order = [rel[(r + k) % 3] for k in range(3)]
            place = jnp.where(turn == r, (order[0] * RING + order[1]) * RING + order[2], place)
        row_of = jnp.where(slots_flat >= 0, (unit * n_experts + place) * BLOCK + within, -1)
        gates = gate_vals.reshape(n_tokens, top_k).T.astype(jnp.float32)
        hidden, normed = attention(x_in.reshape(n_tokens, model_dim), w_qkv, w_out)
        summed = moe_exchange(capacity // BLOCK, normed, hidden, row_of, gates, (w_gate[0], w_up[0], w_down[0]), (ws_gate, ws_up, ws_down))
        return summed.reshape(n_batch, seq_len, model_dim)

    return jax.shard_map(local_step, mesh=mesh, in_specs=(tok_spec, row_spec, row_spec, P("ep", "fsdp", None), P("ep", "fsdp", None), P("ep", None, "fsdp"), row_spec, row_spec, P(None, "fsdp"), tok_spec, tok_spec, tok_spec), out_specs=tok_spec, check_vma=False)
```

```python
import functools

import jax
import jax.numpy as jnp
import numpy as np
from jax import lax
from jax.experimental import pallas as pl
from jax.experimental.pallas import tpu as pltpu
from jax.sharding import PartitionSpec as P

HEAD_DIM = 128
ROPE_BASE = 10000.0
EPSILON = 1e-6
RING = 4
BLOCK = 8
TURNS = 3
WIDE = 256
MESH = pl.DeviceIdType.MESH
STRIDES = (RING * RING, RING, 1)


def rms_norm(values):
    vals_f32 = values.astype(jnp.float32)
    mean_sq = jnp.mean(vals_f32 * vals_f32, axis=-1, keepdims=True)
    return (vals_f32 * lax.rsqrt(mean_sq + EPSILON)).astype(jnp.bfloat16)


def rotary_tables(seq_len):
    half_dim = HEAD_DIM // 2
    inv_freq = (ROPE_BASE ** (-np.arange(half_dim) * (2.0 / HEAD_DIM))).astype(np.float32)
    angles = (np.arange(seq_len, dtype=np.float32)[:, None] * inv_freq[None, :]).astype(np.float64)
    cos_tab, sin_tab = np.cos(angles), np.sin(angles)
    return (np.concatenate([cos_tab, cos_tab], axis=1).astype(np.float32), np.concatenate([-sin_tab, sin_tab], axis=1).astype(np.float32))


def dot32(left, right):
    return jnp.dot(left, right, preferred_element_type=jnp.float32)


def norm_rows(src_ref, dst_ref, group=48):
    def step(g, carry):
        at = pl.ds(pl.multiple_of(g * group, group), group)
        dst_ref[at, :] = rms_norm(src_ref[at, :])
        return carry

    lax.fori_loop(0, src_ref.shape[0] // group, step, 0)


def attention_kernel(x_ref, cos_ref, sin_ref, qkv_hbm, out_hbm, hidden_ref, normed_ref,
                     a_ref, o_ref, own_ref, far_ref, wo_own, wo_far, own_sem, send_sem, recv_sem, wo_sem):
    fs = lax.axis_index("fsdp")
    partner = {"fsdp": 1 - fs}
    seq_len, width = x_ref.shape
    half = width // 2
    n_chunks = width // WIDE
    barrier = pltpu.get_barrier_semaphore()
    pl.semaphore_signal(barrier, inc=1, device_id=partner, device_id_type=MESH)
    pl.semaphore_wait(barrier, 1)
    for c in range(n_chunks):
        for t in range(3):
            cols = qkv_hbm.at[:, pl.ds(t * width + c * WIDE, WIDE)]
            pltpu.make_async_remote_copy(src_ref=cols, dst_ref=far_ref.at[c, t], send_sem=send_sem.at[c], recv_sem=recv_sem.at[c],
                                         device_id=partner, device_id_type=MESH).start()
            pltpu.make_async_copy(cols, own_ref.at[c, t], own_sem.at[c]).start()
    wo_push = pltpu.make_async_remote_copy(src_ref=out_hbm, dst_ref=wo_far, send_sem=send_sem.at[n_chunks], recv_sem=recv_sem.at[n_chunks],
                                           device_id=partner, device_id_type=MESH)
    wo_push.start()
    wo_load = pltpu.make_async_copy(out_hbm, wo_own, wo_sem)
    wo_load.start()
    norm_rows(x_ref, a_ref)

    def own(side):
        return pl.ds(pl.multiple_of(lax.rem(fs + side, 2) * half, half), half)

    def chunk_step(c, carry):
        pltpu.make_async_copy(own_ref.at[c], own_ref.at[c], own_sem.at[c]).wait()
        pltpu.make_async_copy(far_ref.at[c], far_ref.at[c], recv_sem.at[c]).wait()
        left, right = a_ref[:, own(0)], a_ref[:, own(1)]
        q, k, v = [(dot32(left, own_ref[c, t]) + dot32(right, far_ref[c, t])).astype(jnp.bfloat16) for t in range(3)]

        def rotate(vals):
            wide = vals.astype(jnp.float32)
            return (wide * cos_ref[...] + pltpu.roll(wide, HEAD_DIM // 2, 1) * sin_ref[...]).astype(jnp.bfloat16)

        heads = []
        for j in range(WIDE // HEAD_DIM):
            cols = slice(j * HEAD_DIM, (j + 1) * HEAD_DIM)
            query, key, value = rotate(q[:, cols]), rotate(k[:, cols]), v[:, cols]
            parts = []
            for i in range(seq_len // 128):
                span = (i + 1) * 128
                scores = lax.dot_general(query[i * 128:span], key[:span], (((1,), (1,)), ((), ())), preferred_element_type=jnp.float32) * (HEAD_DIM ** -0.5)
                row_at = lax.broadcasted_iota(jnp.int32, (128, span), 0) + i * 128
                col_at = lax.broadcasted_iota(jnp.int32, (128, span), 1)
                scores = jnp.where(row_at >= col_at, scores, -1e30)
                power = jnp.exp(scores - jnp.max(scores, axis=-1, keepdims=True))
                probs = (power / jnp.sum(power, axis=-1, keepdims=True)).astype(jnp.bfloat16)
                parts.append(dot32(probs, value[:span]).astype(jnp.bfloat16))
            heads.append(jnp.concatenate(parts, axis=0))
        o_ref[:, pl.ds(pl.multiple_of(c * WIDE, WIDE), WIDE)] = jnp.concatenate(heads, axis=1)
        return carry

    lax.fori_loop(0, n_chunks, chunk_step, 0)
    wo_load.wait()
    wo_push.wait_recv()

    def out_step(n, carry):
        cols = pl.ds(pl.multiple_of(n * WIDE, WIDE), WIDE)
        mixed = dot32(o_ref[:, own(0)], wo_own[:, cols]) + dot32(o_ref[:, own(1)], wo_far[:, cols])
        hidden_ref[:, cols] = (x_ref[:, cols].astype(jnp.float32) + mixed).astype(jnp.bfloat16)
        return carry

    lax.fori_loop(0, n_chunks, out_step, 0)
    norm_rows(hidden_ref, normed_ref)
    for c in range(n_chunks):
        pltpu.make_async_copy(far_ref.at[c], far_ref.at[c], send_sem.at[c]).wait()
    wo_push.wait_send()


def attention(x_rows, w_qkv, w_out):
    seq_len, width = x_rows.shape
    half, n_chunks = width // 2, width // WIDE
    anywhere = pl.BlockSpec(memory_space=pl.ANY)
    vmem = pl.BlockSpec(memory_space=pltpu.VMEM)
    rows = jax.ShapeDtypeStruct((seq_len, width), jnp.bfloat16)
    sems = pltpu.SemaphoreType.DMA
    cos_tab, sin_tab = rotary_tables(seq_len)
    return pl.pallas_call(
        attention_kernel,
        out_shape=(rows, rows),
        in_specs=[vmem] * 3 + [anywhere] * 2,
        out_specs=(vmem, vmem),
        scratch_shapes=[
            pltpu.VMEM((seq_len, width), jnp.bfloat16),
            pltpu.VMEM((seq_len, width), jnp.bfloat16),
            pltpu.VMEM((n_chunks, 3, half, WIDE), jnp.bfloat16),
            pltpu.VMEM((n_chunks, 3, half, WIDE), jnp.bfloat16),
            pltpu.VMEM(w_out.shape, jnp.bfloat16),
            pltpu.VMEM(w_out.shape, jnp.bfloat16),
            sems((n_chunks,)), sems((n_chunks + 1,)), sems((n_chunks + 1,)), sems(()),
        ],
        compiler_params=pltpu.CompilerParams(collective_id=1, has_side_effects=True, vmem_limit_bytes=56 * 1024 * 1024),
        cost_estimate=pl.CostEstimate(flops=20_000_000_000, bytes_accessed=40_000_000, transcendentals=3_000_000),
        name="attention",
    )(x_rows, jnp.asarray(cos_tab), jnp.asarray(sin_tab), w_qkv, w_out)


def capacity_for(n_tokens, top_k, n_experts):
    return ((5 * n_tokens * top_k) // (4 * n_experts) + 7) // 8 * 8


def ring_peer(me, axis, offset):
    stride = RING * RING - 12 * axis + 9 * (axis * (axis - 1) // 2)
    place = lax.rem(me // stride, RING)
    return me + (lax.rem(place + offset + RING, RING) - place) * stride


class Exchange:
    def __init__(self, me, axes, sign, unit, buffers, send, recv):
        self.me, self.axes, self.sign = me, axes, sign
        self.first, self.second, self.third, self.last = [ref.at[unit] for ref in buffers]
        self.send, self.recv = send.at[unit], recv.at[unit]

    def push(self, phase, d):
        peer = ring_peer(self.me, self.axes[phase], self.sign * d)
        if phase == 0:
            pairs = [(self.first.at[d], self.second.at[:, :, d - 1])]
        elif phase == 1:
            pairs = [(self.first.at[0, d], self.third.at[:, d - 1, 0]), (self.second.at[d], self.third.at[:, d - 1, pl.ds(1, 3)])]
        else:
            pairs = [(self.first.at[0, 0, d], self.last.at[d - 1, 0, 0]), (self.second.at[0, d], self.last.at[d - 1, 0, pl.ds(1, 3)]),
                     (self.third.at[d], self.last.at[d - 1, pl.ds(1, 3)])]
        sem = phase if phase < 2 else 1 + d
        for src, dst in pairs:
            pltpu.make_async_remote_copy(src_ref=src, dst_ref=dst, send_sem=self.send.at[sem], recv_sem=self.recv.at[sem],
                                         device_id={"ep": peer}, device_id_type=MESH).start()

    def start(self, phase):
        for d in (1, 3, 2):
            self.push(phase, d)

    def wait_recv(self, phase):
        whole = (self.second, self.third)[phase]
        pltpu.make_async_copy(whole, whole, self.recv.at[phase]).wait()

    def wait_last(self, d):
        pltpu.make_async_copy(self.last.at[d - 1], self.last.at[d - 1], self.recv.at[1 + d]).wait()

    def wait_sent(self):
        for phase, whole in enumerate((self.second, self.third)):
            pltpu.make_async_copy(whole, whole, self.send.at[phase]).wait()
        for d in range(1, RING):
            pltpu.make_async_copy(self.last.at[d - 1], self.last.at[d - 1], self.send.at[1 + d]).wait()

    def kept(self):
        return [(self.third.at[0], (0, pl.ds(1, 3))), (self.second.at[0, 0], (0, 0, pl.ds(1, 3))), (self.first.at[0, 0, 0], (0, 0, 0))]


def moe_kernel(n_units, normed_ref, hidden_ref, place_ref, weight_ref,
               gate_a, up_a, down_a, sgate_a, sup_a, sdown_a, sum_ref,
               sgate_b, sup_b, sdown_b, rows_hbm, out1, out2, out3, made_hbm, back1, back2, back3,
               ga, gb, ua, ub, da, db, sin_ref, sdn_ref, x_ref, act_ref, y_ref, total_ref, mix_ref, pick_ref,
               w_sem, pair_send, pair_recv, far_send, far_recv, s_sem, x_sem, y_sem, go_send, go_recv, come_send, come_recv):
    me = lax.axis_index("ep")
    fs = lax.axis_index("fsdp")
    barrier = pltpu.get_barrier_semaphore()
    for axis in range(3):
        for d in range(1, RING):
            pl.semaphore_signal(barrier, inc=1, device_id={"ep": ring_peer(me, axis, d)}, device_id_type=MESH)
    partner = {"fsdp": 1 - fs}
    pl.semaphore_signal(barrier, inc=1, device_id=partner, device_id_type=MESH)
    pl.semaphore_wait(barrier, 3 * (RING - 1) + 1)

    half = ga.shape[0]
    inner = ga.shape[1]
    rows = RING ** 3 * BLOCK
    n_tokens = normed_ref.shape[0]
    top_k = place_ref.shape[0]

    def go(u):
        return Exchange(me, [lax.rem(u + k, 3) for k in range(3)], 1, u, (rows_hbm, out1, out2, out3), go_send, go_recv)

    def come(u):
        return Exchange(me, [lax.rem(u + 2 - k, 3) for k in range(3)], -1, u, (made_hbm, back1, back2, back3), come_send, come_recv)

    def advance(exchange, phase):
        exchange.wait_recv(phase)
        exchange.start(phase + 1)

    def each(low, high, step):
        def body(u, carry):
            step(u)
            return carry

        lax.fori_loop(low, high, body, 0)

    def own(side):
        return pl.ds(pl.multiple_of(lax.rem(fs + side, 2) * half, half), half)

    def own_block(side, n):
        return pl.ds(pl.multiple_of(lax.rem(fs + side, 2) * half + n * WIDE, WIDE), WIDE)

    def block_at(n):
        return pl.ds(pl.multiple_of(n * WIDE, WIDE), WIDE)

    def shared_copies(n, slot):
        pairs = [(src, sin_ref.at[slot, k]) for k, src in enumerate((sgate_a.at[:, block_at(n)], sgate_b.at[n], sup_a.at[:, block_at(n)], sup_b.at[n]))]
        pairs += [(src.at[block_at(n)], sdn_ref.at[slot, k]) for k, src in enumerate((sdown_a, sdown_b))]
        return [pltpu.make_async_copy(src, dst, s_sem.at[slot, k]) for k, (src, dst) in enumerate(pairs)]

    def shared_push(n):
        pairs = [(sgate_a.at[:, block_at(n)], sgate_b.at[n]), (sup_a.at[:, block_at(n)], sup_b.at[n]), (sdown_a.at[block_at(n)], sdown_b.at[block_at(n)])]
        return [pltpu.make_async_remote_copy(src_ref=src, dst_ref=dst, send_sem=pair_send.at[k, n], recv_sem=pair_recv.at[k, n],
                                             device_id=partner, device_id_type=MESH) for k, (src, dst) in enumerate(pairs)]

    n_shared = sgate_a.shape[1] // WIDE
    ahead = 3
    for n in range(ahead):
        for copy in shared_push(n):
            copy.start()

    def pick(u):
        slot = lax.rem(u, 2)
        for c in range(rows // 128):
            at = lax.broadcasted_iota(jnp.int32, (128, n_tokens), 0) + (u * rows + c * 128)
            part = jnp.zeros((128, n_tokens), jnp.float32)
            for k in range(top_k):
                part += jnp.where(place_ref[k:k + 1, :] == at, 1.0, 0.0)
            pick_ref[c * 128:(c + 1) * 128, :] = part.astype(jnp.bfloat16)
        x2 = x_ref.at[slot].reshape(rows, 2 * half)

        def pick_step(n, carry):
            x2[:, block_at(n)] = dot32(pick_ref[...], normed_ref[:, block_at(n)]).astype(jnp.bfloat16)
            return carry

        lax.fori_loop(0, 2 * half // WIDE, pick_step, 0)
        copy = pltpu.make_async_copy(x_ref.at[slot], rows_hbm.at[u], y_sem.at[slot, 0])
        copy.start()
        copy.wait()
        go(u).start(0)

    each(0, n_units, pick)
    weights = [pltpu.make_async_copy(src, dst, w_sem.at[n]) for n, (src, dst) in enumerate(((gate_a, ga), (up_a, ua), (down_a, da)))]
    far_weights = [pltpu.make_async_remote_copy(src_ref=src, dst_ref=dst, send_sem=far_send.at[n], recv_sem=far_recv.at[n], device_id=partner, device_id_type=MESH)
                   for n, (src, dst) in enumerate(((gate_a, gb), (up_a, ub), (down_a, db)))]
    for copy in weights:
        copy.start()
    for copy in shared_push(0):
        copy.wait_recv()
    for copy in shared_copies(0, 0):
        copy.start()
    total_ref[...] = hidden_ref[...].astype(jnp.float32)

    def shared_step(n, carry):
        slot = lax.rem(n, 2)
        for copy in shared_copies(n, slot):
            copy.wait()

        @pl.when(n == 4)
        def _():
            each(0, TURNS, lambda u: advance(go(u), 0))

        @pl.when(n + ahead < n_shared)
        def _():
            for copy in shared_push(n + ahead):
                copy.start()

        @pl.when(n + 1 < n_shared)
        def _():
            for copy in shared_push(n + 1):
                copy.wait_recv()
            for copy in shared_copies(n + 1, 1 - slot):
                copy.start()

        left, right = normed_ref[:, own(0)], normed_ref[:, own(1)]
        gate = dot32(left, sin_ref[slot, 0]) + dot32(right, sin_ref[slot, 1])
        up = dot32(left, sin_ref[slot, 2]) + dot32(right, sin_ref[slot, 3])
        act_ref[pl.ds(0, n_tokens), pl.ds(0, WIDE)] = (jax.nn.silu(gate) * up).astype(jnp.bfloat16)

        def shared_down(m, c):
            for side in range(2):
                total_ref[:, own_block(side, m)] += dot32(act_ref[pl.ds(0, n_tokens), pl.ds(0, WIDE)], sdn_ref[slot, side, :, block_at(m)])
            return c

        lax.fori_loop(0, half // WIDE, shared_down, 0)
        return carry

    lax.fori_loop(0, n_shared, shared_step, 0)
    for copy in far_weights:
        copy.start()

    each(TURNS, n_units, lambda u: advance(go(u), 0))
    each(0, TURNS, lambda u: advance(go(u), 1))
    for copy in weights:
        copy.wait()
    for copy in far_weights:
        copy.wait_recv()

    tile = TURNS * RING * RING * BLOCK
    top = pl.ds(0, tile)

    def inner_part(slot):
        x2 = x_ref.at[slot].reshape(rows, 2 * half)

        def inner_block(cols):
            gate = dot32(x2[top, own(0)], ga[:, cols]) + dot32(x2[top, own(1)], gb[:, cols])
            up = dot32(x2[top, own(0)], ua[:, cols]) + dot32(x2[top, own(1)], ub[:, cols])
            act_ref[top, cols] = (jax.nn.silu(gate) * up).astype(jnp.bfloat16)

        def inner_step(n, carry):
            inner_block(block_at(n))
            return carry

        whole = inner // WIDE
        lax.fori_loop(0, whole, inner_step, 0)
        if inner % WIDE:
            inner_block(pl.ds(whole * WIDE, inner % WIDE))

    def down_part(slot):
        y2 = y_ref.at[slot].reshape(tile, 2 * half)

        def down_step(n, carry):
            for side, weight in enumerate((da, db)):
                y2[:, own_block(side, n)] = dot32(act_ref[top, :], weight[:, block_at(n)]).astype(jnp.bfloat16)
            return carry

        lax.fori_loop(0, half // WIDE, down_step, 0)

    def put(b, d, slot):
        copies = [pltpu.make_async_copy(y_ref.at[slot, r], made_hbm.at[b * TURNS + r, d], y_sem.at[slot, r]) for r in range(TURNS)]
        for copy in copies:
            copy.start()
        for copy in copies:
            copy.wait()

    def near_tile(b):
        copies = []
        for r in range(TURNS):
            for n, (src, place) in enumerate(go(b * TURNS + r).kept()):
                copies.append(pltpu.make_async_copy(src, x_ref.at[(b, r, *place[1:])], x_sem.at[b, 3 * r + n]))
        for copy in copies:
            copy.start()
        for copy in copies:
            copy.wait()
        inner_part(b)
        down_part(b)
        put(b, 0, b)

    def far_of(s):
        j = lax.rem(s, 3)
        return s // 3, j, 1 + 2 * j - 3 * (j // 2)

    def far_loads(s, slot):
        b, _, d = far_of(s)
        return [pltpu.make_async_copy(go(b * TURNS + r).last.at[d - 1], x_ref.at[slot, r], x_sem.at[slot, r]) for r in range(TURNS)]

    def begin(s, slot):
        b, _, d = far_of(s)
        for r in range(TURNS):
            go(b * TURNS + r).wait_last(d)
        for copy in far_loads(s, slot):
            copy.start()

    def far_tile(s):
        slot = lax.rem(s, 2)
        b, j, d = far_of(s)

        @pl.when(j == 0)
        def _():
            begin(s, slot)

        for copy in far_loads(s, slot):
            copy.wait()
        inner_part(slot)

        @pl.when(j < 2)
        def _():
            begin(s + 1, 1 - slot)

        down_part(slot)
        put(b, d, slot)
        for r in range(TURNS):
            come(b * TURNS + r).push(0, d)

        @pl.when(s == 4)
        def _():
            each(0, TURNS, lambda u: advance(come(u), 0))

    near_tile(0)
    each(TURNS, n_units, lambda u: advance(go(u), 1))
    near_tile(1)
    each(0, n_units, far_tile)
    each(0, TURNS, lambda u: advance(come(u), 1))
    each(TURNS, n_units, lambda u: advance(come(u), 0))
    each(TURNS, n_units, lambda u: advance(come(u), 1))

    def loads(exchange, slot):
        pieces = [(exchange.last, (pl.ds(1, 3),))] + exchange.kept()
        return [pltpu.make_async_copy(src, x_ref.at[(slot, *place)], x_sem.at[slot, n]) for n, (src, place) in enumerate(pieces)]

    def fetch(exchange, slot):
        for d in range(1, RING):
            exchange.wait_last(d)
        for copy in loads(exchange, slot):
            copy.start()

    fetch(come(0), 0)

    def mix(u):
        slot = lax.rem(u, 2)
        for c in range(rows // 128):
            at = lax.broadcasted_iota(jnp.int32, (128, n_tokens), 0) + (u * rows + c * 128)
            part = jnp.zeros((128, n_tokens), jnp.float32)
            for k in range(top_k):
                part += jnp.where(place_ref[k:k + 1, :] == at, weight_ref[k:k + 1, :], 0.0)
            mix_ref[:, c * 128:(c + 1) * 128] = part.T.astype(jnp.bfloat16)
        for copy in loads(come(u), slot):
            copy.wait()

        @pl.when(u + 1 < n_units)
        def _():
            fetch(come(u + 1), 1 - slot)

        x2 = x_ref.at[slot].reshape(rows, 2 * half)

        def mix_step(n, carry):
            total_ref[:, block_at(n)] += dot32(mix_ref[...], x2[:, block_at(n)])
            return carry

        lax.fori_loop(0, 2 * half // WIDE, mix_step, 0)

    each(0, n_units, mix)
    sum_ref[...] = total_ref[...].astype(jnp.bfloat16)
    for copy in far_weights:
        copy.wait_send()

    def pair_done(n, carry):
        for copy in shared_push(n):
            copy.wait_send()
        return carry

    lax.fori_loop(0, n_shared, pair_done, 0)

    def sent(u):
        go(u).wait_sent()
        come(u).wait_sent()

    each(0, n_units, sent)


def moe_exchange(n_units, normed, hidden, place, weight, weights, shared):
    n_tokens, width = normed.shape
    anywhere = pl.BlockSpec(memory_space=pl.ANY)
    vmem = pl.BlockSpec(memory_space=pltpu.VMEM)
    inner, n_shared = weights[0].shape[1], shared[0].shape[1] // WIDE

    def blocks(*lead):
        return jax.ShapeDtypeStruct((n_units, *lead, BLOCK, width), jnp.bfloat16)

    cube = (RING, RING, RING, BLOCK, width)
    steps = [blocks(4, 4, 3), blocks(4, 3, 4), blocks(3, 4, 4)]
    wide_block = jax.ShapeDtypeStruct((n_shared, width // 2, WIDE), jnp.bfloat16)
    far = [wide_block, wide_block, jax.ShapeDtypeStruct(shared[2].shape, jnp.bfloat16)]
    outs = [jax.ShapeDtypeStruct((n_tokens, width), jnp.bfloat16)] + far + [blocks(4, 4, 4)] + steps + [blocks(4, 4, 4)] + steps
    sems = pltpu.SemaphoreType.DMA
    return pl.pallas_call(
        functools.partial(moe_kernel, n_units),
        out_shape=tuple(outs),
        in_specs=[vmem] * 4 + [anywhere] * 6,
        out_specs=(vmem,) + (anywhere,) * 11,
        scratch_shapes=[pltpu.VMEM(w.shape, jnp.bfloat16) for w in weights for _ in range(2)] + [
            pltpu.VMEM((2, 4, width // 2, WIDE), jnp.bfloat16),
            pltpu.VMEM((2, 2, WIDE, width // 2), jnp.bfloat16),
            pltpu.VMEM((2, *cube), jnp.bfloat16),
            pltpu.VMEM((RING ** 3 * BLOCK, inner), jnp.bfloat16),
            pltpu.VMEM((2, TURNS, *cube[1:]), jnp.bfloat16),
            pltpu.VMEM((n_tokens, width), jnp.float32),
            pltpu.VMEM((n_tokens, RING ** 3 * BLOCK), jnp.bfloat16),
            pltpu.VMEM((RING ** 3 * BLOCK, n_tokens), jnp.bfloat16),
            sems((3,)), sems((3, n_shared)), sems((3, n_shared)), sems((3,)), sems((3,)), sems((2, 6)), sems((2, 9)), sems((2, 3)),
            sems((n_units, 5)), sems((n_units, 5)), sems((n_units, 5)), sems((n_units, 5)),
        ],
        compiler_params=pltpu.CompilerParams(collective_id=0, has_side_effects=True, vmem_limit_bytes=60 * 1024 * 1024),
        cost_estimate=pl.CostEstimate(flops=250_000_000_000, bytes_accessed=100_000_000, transcendentals=0),
        name="moe_exchange",
    )(normed, hidden, place, weight, *weights, *shared)[0]


def solution(mesh):
    n_ep = mesh.shape["ep"]
    tok_spec = P(("data", "fsdp", "ep"))
    row_spec = P("fsdp", None)

    def local_step(x_in, w_qkv, w_out, w_gate, w_up, w_down, ws_gate, ws_up, ws_down, expert_ids, slot_ids, gate_vals):
        n_batch, seq_len, model_dim = x_in.shape
        n_tokens = n_batch * seq_len
        top_k = expert_ids.shape[-1]
        n_experts = w_gate.shape[0] * n_ep
        capacity = capacity_for(n_tokens, top_k, n_experts)
        ids_flat = expert_ids.reshape(n_tokens, top_k).T
        slots_flat = slot_ids.reshape(n_tokens, top_k).T
        me = lax.axis_index("ep")
        rel = [lax.rem(ids_flat // s - me // s + n_ep, RING) for s in STRIDES]
        unit, within = slots_flat // BLOCK, slots_flat % BLOCK
        turn = unit % TURNS
        place = jnp.zeros_like(slots_flat)
        for r in range(TURNS):
            order = [rel[(r + k) % 3] for k in range(3)]
            place = jnp.where(turn == r, (order[0] * RING + order[1]) * RING + order[2], place)
        row_of = jnp.where(slots_flat >= 0, (unit * n_experts + place) * BLOCK + within, -1)
        gates = gate_vals.reshape(n_tokens, top_k).T.astype(jnp.float32)
        hidden, normed = attention(x_in.reshape(n_tokens, model_dim), w_qkv, w_out)
        summed = moe_exchange(capacity // BLOCK, normed, hidden, row_of, gates, (w_gate[0], w_up[0], w_down[0]), (ws_gate, ws_up, ws_down))
        return summed.reshape(n_batch, seq_len, model_dim)

    return jax.shard_map(local_step, mesh=mesh, in_specs=(tok_spec, row_spec, row_spec, P("ep", "fsdp", None), P("ep", "fsdp", None), P("ep", None, "fsdp"), row_spec, row_spec, P(None, "fsdp"), tok_spec, tok_spec, tok_spec), out_specs=tok_spec, check_vma=False)
```

```python
import functools

import jax
import jax.numpy as jnp
import numpy as np
from jax import lax
from jax.experimental import pallas as pl
from jax.experimental.pallas import tpu as pltpu
from jax.sharding import PartitionSpec as P

HEAD_DIM = 128
ROPE_BASE = 10000.0
EPSILON = 1e-6
RING = 4
BLOCK = 8
TURNS = 3
WIDE = 256
MESH = pl.DeviceIdType.MESH
STRIDES = (RING * RING, RING, 1)


def rms_norm(values):
    vals_f32 = values.astype(jnp.float32)
    mean_sq = jnp.mean(vals_f32 * vals_f32, axis=-1, keepdims=True)
    return (vals_f32 * lax.rsqrt(mean_sq + EPSILON)).astype(jnp.bfloat16)


def rotary_tables(seq_len):
    half_dim = HEAD_DIM // 2
    inv_freq = (ROPE_BASE ** (-np.arange(half_dim) * (2.0 / HEAD_DIM))).astype(np.float32)
    angles = (np.arange(seq_len, dtype=np.float32)[:, None] * inv_freq[None, :]).astype(np.float64)
    cos_tab, sin_tab = np.cos(angles), np.sin(angles)
    return (np.concatenate([cos_tab, cos_tab], axis=1).astype(np.float32), np.concatenate([-sin_tab, sin_tab], axis=1).astype(np.float32))


def dot32(left, right):
    return jnp.dot(left, right, preferred_element_type=jnp.float32)


def norm_rows(src_ref, dst_ref, group=48):
    def step(g, carry):
        at = pl.ds(pl.multiple_of(g * group, group), group)
        dst_ref[at, :] = rms_norm(src_ref[at, :])
        return carry

    lax.fori_loop(0, src_ref.shape[0] // group, step, 0)


def attention_kernel(x_ref, cos_ref, sin_ref, qkv_hbm, out_hbm, hidden_ref, normed_ref,
                     a_ref, o_ref, own_ref, far_ref, wo_own, wo_far, own_sem, send_sem, recv_sem, wo_sem):
    fs = lax.axis_index("fsdp")
    partner = {"fsdp": 1 - fs}
    seq_len, width = x_ref.shape
    half = width // 2
    n_chunks = width // WIDE
    barrier = pltpu.get_barrier_semaphore()
    pl.semaphore_signal(barrier, inc=1, device_id=partner, device_id_type=MESH)
    pl.semaphore_wait(barrier, 1)
    for c in range(n_chunks):
        for t in range(3):
            cols = qkv_hbm.at[:, pl.ds(t * width + c * WIDE, WIDE)]
            pltpu.make_async_remote_copy(src_ref=cols, dst_ref=far_ref.at[c, t], send_sem=send_sem.at[c], recv_sem=recv_sem.at[c],
                                         device_id=partner, device_id_type=MESH).start()
            pltpu.make_async_copy(cols, own_ref.at[c, t], own_sem.at[c]).start()
    wo_push = pltpu.make_async_remote_copy(src_ref=out_hbm, dst_ref=wo_far, send_sem=send_sem.at[n_chunks], recv_sem=recv_sem.at[n_chunks],
                                           device_id=partner, device_id_type=MESH)
    wo_push.start()
    wo_load = pltpu.make_async_copy(out_hbm, wo_own, wo_sem)
    wo_load.start()
    norm_rows(x_ref, a_ref)

    def own(side):
        return pl.ds(pl.multiple_of(lax.rem(fs + side, 2) * half, half), half)

    def project(c):
        left, right = a_ref[:, own(0)], a_ref[:, own(1)]
        return [(dot32(left, own_ref[c, t]) + dot32(right, far_ref[c, t])).astype(jnp.bfloat16) for t in range(3)]

    def chunk_step(pair, carry):
        for c in (2 * pair, 2 * pair + 1):
            pltpu.make_async_copy(own_ref.at[c], own_ref.at[c], own_sem.at[c]).wait()
            pltpu.make_async_copy(far_ref.at[c], far_ref.at[c], recv_sem.at[c]).wait()
        ready = [project(2 * pair + n) for n in range(2)]

        def rotate(vals):
            wide = vals.astype(jnp.float32)
            return (wide * cos_ref[...] + pltpu.roll(wide, HEAD_DIM // 2, 1) * sin_ref[...]).astype(jnp.bfloat16)

        for n, (q, k, v) in enumerate(ready):
            heads = []
            for j in range(WIDE // HEAD_DIM):
                cols = slice(j * HEAD_DIM, (j + 1) * HEAD_DIM)
                query, key, value = rotate(q[:, cols]), rotate(k[:, cols]), v[:, cols]
                parts = []
                for i in range(seq_len // 128):
                    span = (i + 1) * 128
                    scores = lax.dot_general(query[i * 128:span], key[:span], (((1,), (1,)), ((), ())), preferred_element_type=jnp.float32) * (HEAD_DIM ** -0.5)
                    row_at = lax.broadcasted_iota(jnp.int32, (128, span), 0) + i * 128
                    col_at = lax.broadcasted_iota(jnp.int32, (128, span), 1)
                    scores = jnp.where(row_at >= col_at, scores, -1e30)
                    power = jnp.exp(scores - jnp.max(scores, axis=-1, keepdims=True))
                    probs = (power / jnp.sum(power, axis=-1, keepdims=True)).astype(jnp.bfloat16)
                    parts.append(dot32(probs, value[:span]).astype(jnp.bfloat16))
                heads.append(jnp.concatenate(parts, axis=0))
            o_ref[:, pl.ds(pl.multiple_of((2 * pair + n) * WIDE, WIDE), WIDE)] = jnp.concatenate(heads, axis=1)
        return carry

    lax.fori_loop(0, n_chunks // 2, chunk_step, 0)
    wo_load.wait()
    wo_push.wait_recv()

    def out_step(n, carry):
        cols = pl.ds(pl.multiple_of(n * WIDE, WIDE), WIDE)
        mixed = dot32(o_ref[:, own(0)], wo_own[:, cols]) + dot32(o_ref[:, own(1)], wo_far[:, cols])
        hidden_ref[:, cols] = (x_ref[:, cols].astype(jnp.float32) + mixed).astype(jnp.bfloat16)
        return carry

    lax.fori_loop(0, n_chunks, out_step, 0)
    norm_rows(hidden_ref, normed_ref)
    for c in range(n_chunks):
        pltpu.make_async_copy(far_ref.at[c], far_ref.at[c], send_sem.at[c]).wait()
    wo_push.wait_send()


def attention(x_rows, w_qkv, w_out):
    seq_len, width = x_rows.shape
    half, n_chunks = width // 2, width // WIDE
    anywhere = pl.BlockSpec(memory_space=pl.ANY)
    vmem = pl.BlockSpec(memory_space=pltpu.VMEM)
    rows = jax.ShapeDtypeStruct((seq_len, width), jnp.bfloat16)
    sems = pltpu.SemaphoreType.DMA
    cos_tab, sin_tab = rotary_tables(seq_len)
    return pl.pallas_call(
        attention_kernel,
        out_shape=(rows, rows),
        in_specs=[vmem] * 3 + [anywhere] * 2,
        out_specs=(vmem, vmem),
        scratch_shapes=[
            pltpu.VMEM((seq_len, width), jnp.bfloat16),
            pltpu.VMEM((seq_len, width), jnp.bfloat16),
            pltpu.VMEM((n_chunks, 3, half, WIDE), jnp.bfloat16),
            pltpu.VMEM((n_chunks, 3, half, WIDE), jnp.bfloat16),
            pltpu.VMEM(w_out.shape, jnp.bfloat16),
            pltpu.VMEM(w_out.shape, jnp.bfloat16),
            sems((n_chunks,)), sems((n_chunks + 1,)), sems((n_chunks + 1,)), sems(()),
        ],
        compiler_params=pltpu.CompilerParams(collective_id=1, has_side_effects=True, vmem_limit_bytes=56 * 1024 * 1024),
        cost_estimate=pl.CostEstimate(flops=20_000_000_000, bytes_accessed=40_000_000, transcendentals=3_000_000),
        name="attention",
    )(x_rows, jnp.asarray(cos_tab), jnp.asarray(sin_tab), w_qkv, w_out)


def capacity_for(n_tokens, top_k, n_experts):
    return ((5 * n_tokens * top_k) // (4 * n_experts) + 7) // 8 * 8


def ring_peer(me, axis, offset):
    stride = RING * RING - 12 * axis + 9 * (axis * (axis - 1) // 2)
    place = lax.rem(me // stride, RING)
    return me + (lax.rem(place + offset + RING, RING) - place) * stride


class Exchange:
    def __init__(self, me, axes, sign, unit, buffers, send, recv):
        self.me, self.axes, self.sign = me, axes, sign
        self.first, self.second, self.third, self.last = [ref.at[unit] for ref in buffers]
        self.send, self.recv = send.at[unit], recv.at[unit]

    def push(self, phase, d):
        peer = ring_peer(self.me, self.axes[phase], self.sign * d)
        if phase == 0:
            pairs = [(self.first.at[d], self.second.at[:, :, d - 1])]
        elif phase == 1:
            pairs = [(self.first.at[0, d], self.third.at[:, d - 1, 0]), (self.second.at[d], self.third.at[:, d - 1, pl.ds(1, 3)])]
        else:
            pairs = [(self.first.at[0, 0, d], self.last.at[d - 1, 0, 0]), (self.second.at[0, d], self.last.at[d - 1, 0, pl.ds(1, 3)]),
                     (self.third.at[d], self.last.at[d - 1, pl.ds(1, 3)])]
        sem = phase if phase < 2 else 1 + d
        for src, dst in pairs:
            pltpu.make_async_remote_copy(src_ref=src, dst_ref=dst, send_sem=self.send.at[sem], recv_sem=self.recv.at[sem],
                                         device_id={"ep": peer}, device_id_type=MESH).start()

    def start(self, phase):
        for d in (1, 3, 2):
            self.push(phase, d)

    def wait_recv(self, phase):
        whole = (self.second, self.third)[phase]
        pltpu.make_async_copy(whole, whole, self.recv.at[phase]).wait()

    def wait_last(self, d):
        pltpu.make_async_copy(self.last.at[d - 1], self.last.at[d - 1], self.recv.at[1 + d]).wait()

    def wait_sent(self):
        for phase, whole in enumerate((self.second, self.third)):
            pltpu.make_async_copy(whole, whole, self.send.at[phase]).wait()
        for d in range(1, RING):
            pltpu.make_async_copy(self.last.at[d - 1], self.last.at[d - 1], self.send.at[1 + d]).wait()

    def kept(self):
        return [(self.third.at[0], (0, pl.ds(1, 3))), (self.second.at[0, 0], (0, 0, pl.ds(1, 3))), (self.first.at[0, 0, 0], (0, 0, 0))]


def moe_kernel(n_units, normed_ref, hidden_ref, place_ref, weight_ref,
               gate_a, up_a, down_a, sgate_a, sup_a, sdown_a, sum_ref,
               sgate_b, sup_b, sdown_b, rows_hbm, out1, out2, out3, made_hbm, back1, back2, back3,
               ga, gb, ua, ub, da, db, sin_ref, sdn_ref, x_ref, act_ref, y_ref, total_ref, mix_ref, pick_ref,
               w_sem, pair_send, pair_recv, far_send, far_recv, s_sem, x_sem, y_sem, go_send, go_recv, come_send, come_recv):
    me = lax.axis_index("ep")
    fs = lax.axis_index("fsdp")
    barrier = pltpu.get_barrier_semaphore()
    for axis in range(3):
        for d in range(1, RING):
            pl.semaphore_signal(barrier, inc=1, device_id={"ep": ring_peer(me, axis, d)}, device_id_type=MESH)
    partner = {"fsdp": 1 - fs}
    pl.semaphore_signal(barrier, inc=1, device_id=partner, device_id_type=MESH)
    pl.semaphore_wait(barrier, 3 * (RING - 1) + 1)

    half = ga.shape[0]
    inner = ga.shape[1]
    rows = RING ** 3 * BLOCK
    n_tokens = normed_ref.shape[0]
    top_k = place_ref.shape[0]

    def go(u):
        return Exchange(me, [lax.rem(u + k, 3) for k in range(3)], 1, u, (rows_hbm, out1, out2, out3), go_send, go_recv)

    def come(u):
        return Exchange(me, [lax.rem(u + 2 - k, 3) for k in range(3)], -1, u, (made_hbm, back1, back2, back3), come_send, come_recv)

    def advance(exchange, phase):
        exchange.wait_recv(phase)
        exchange.start(phase + 1)

    def each(low, high, step):
        def body(u, carry):
            step(u)
            return carry

        lax.fori_loop(low, high, body, 0)

    def own(side):
        return pl.ds(pl.multiple_of(lax.rem(fs + side, 2) * half, half), half)

    def own_block(side, n):
        return pl.ds(pl.multiple_of(lax.rem(fs + side, 2) * half + n * WIDE, WIDE), WIDE)

    def block_at(n):
        return pl.ds(pl.multiple_of(n * WIDE, WIDE), WIDE)

    def shared_copies(n, slot):
        pairs = [(src, sin_ref.at[slot, k]) for k, src in enumerate((sgate_a.at[:, block_at(n)], sgate_b.at[n], sup_a.at[:, block_at(n)], sup_b.at[n]))]
        pairs += [(src.at[block_at(n)], sdn_ref.at[slot, k]) for k, src in enumerate((sdown_a, sdown_b))]
        return [pltpu.make_async_copy(src, dst, s_sem.at[slot, k]) for k, (src, dst) in enumerate(pairs)]

    def shared_push(n):
        pairs = [(sgate_a.at[:, block_at(n)], sgate_b.at[n]), (sup_a.at[:, block_at(n)], sup_b.at[n]), (sdown_a.at[block_at(n)], sdown_b.at[block_at(n)])]
        return [pltpu.make_async_remote_copy(src_ref=src, dst_ref=dst, send_sem=pair_send.at[k, n], recv_sem=pair_recv.at[k, n],
                                             device_id=partner, device_id_type=MESH) for k, (src, dst) in enumerate(pairs)]

    n_shared = sgate_a.shape[1] // WIDE
    ahead = 3
    for n in range(ahead):
        for copy in shared_push(n):
            copy.start()

    def pick_copy(u):
        slot = lax.rem(u, 2)
        return pltpu.make_async_copy(x_ref.at[slot], rows_hbm.at[u], y_sem.at[slot, 0])

    def flush(u):
        pick_copy(u).wait()
        go(u).start(0)

    def pick(u):
        slot = lax.rem(u, 2)
        for c in range(rows // 128):
            at = lax.broadcasted_iota(jnp.int32, (128, n_tokens), 0) + (u * rows + c * 128)
            part = jnp.zeros((128, n_tokens), jnp.float32)
            for k in range(top_k):
                part += jnp.where(place_ref[k:k + 1, :] == at, 1.0, 0.0)
            pick_ref[c * 128:(c + 1) * 128, :] = part.astype(jnp.bfloat16)
        x2 = x_ref.at[slot].reshape(rows, 2 * half)

        def pick_step(n, carry):
            x2[:, block_at(n)] = dot32(pick_ref[...], normed_ref[:, block_at(n)]).astype(jnp.bfloat16)
            return carry

        lax.fori_loop(0, 2 * half // WIDE, pick_step, 0)
        @pl.when(u >= 1)
        def _():
            flush(u - 1)

        pick_copy(u).start()

    each(0, n_units, pick)
    flush(n_units - 1)
    weights = [pltpu.make_async_copy(src, dst, w_sem.at[n]) for n, (src, dst) in enumerate(((gate_a, ga), (up_a, ua), (down_a, da)))]
    far_weights = [pltpu.make_async_remote_copy(src_ref=src, dst_ref=dst, send_sem=far_send.at[n], recv_sem=far_recv.at[n], device_id=partner, device_id_type=MESH)
                   for n, (src, dst) in enumerate(((gate_a, gb), (up_a, ub), (down_a, db)))]
    for copy in weights:
        copy.start()
    for copy in shared_push(0):
        copy.wait_recv()
    for copy in shared_copies(0, 0):
        copy.start()
    total_ref[...] = hidden_ref[...].astype(jnp.float32)

    def shared_step(n, carry):
        slot = lax.rem(n, 2)
        for copy in shared_copies(n, slot):
            copy.wait()

        @pl.when(n == 4)
        def _():
            each(0, TURNS, lambda u: advance(go(u), 0))

        @pl.when(n + ahead < n_shared)
        def _():
            for copy in shared_push(n + ahead):
                copy.start()

        @pl.when(n + 1 < n_shared)
        def _():
            for copy in shared_push(n + 1):
                copy.wait_recv()
            for copy in shared_copies(n + 1, 1 - slot):
                copy.start()

        left, right = normed_ref[:, own(0)], normed_ref[:, own(1)]
        gate = dot32(left, sin_ref[slot, 0]) + dot32(right, sin_ref[slot, 1])
        up = dot32(left, sin_ref[slot, 2]) + dot32(right, sin_ref[slot, 3])
        act_ref[pl.ds(0, n_tokens), pl.ds(0, WIDE)] = (jax.nn.silu(gate) * up).astype(jnp.bfloat16)

        def shared_down(m, c):
            for side in range(2):
                total_ref[:, own_block(side, m)] += dot32(act_ref[pl.ds(0, n_tokens), pl.ds(0, WIDE)], sdn_ref[slot, side, :, block_at(m)])
            return c

        lax.fori_loop(0, half // WIDE, shared_down, 0)
        return carry

    lax.fori_loop(0, n_shared, shared_step, 0)
    for copy in far_weights:
        copy.start()

    each(TURNS, n_units, lambda u: advance(go(u), 0))
    each(0, TURNS, lambda u: advance(go(u), 1))
    for copy in weights:
        copy.wait()
    for copy in far_weights:
        copy.wait_recv()

    tile = TURNS * RING * RING * BLOCK
    top = pl.ds(0, tile)

    def inner_part(slot):
        x2 = x_ref.at[slot].reshape(rows, 2 * half)

        def inner_block(cols):
            gate = dot32(x2[top, own(0)], ga[:, cols]) + dot32(x2[top, own(1)], gb[:, cols])
            up = dot32(x2[top, own(0)], ua[:, cols]) + dot32(x2[top, own(1)], ub[:, cols])
            act_ref[top, cols] = (jax.nn.silu(gate) * up).astype(jnp.bfloat16)

        def inner_step(n, carry):
            inner_block(block_at(n))
            return carry

        whole = inner // WIDE
        lax.fori_loop(0, whole, inner_step, 0)
        if inner % WIDE:
            inner_block(pl.ds(whole * WIDE, inner % WIDE))

    def down_part(slot):
        y2 = y_ref.at[slot].reshape(tile, 2 * half)

        def down_step(n, carry):
            for side, weight in enumerate((da, db)):
                y2[:, own_block(side, n)] = dot32(act_ref[top, :], weight[:, block_at(n)]).astype(jnp.bfloat16)
            return carry

        lax.fori_loop(0, half // WIDE, down_step, 0)

    def put(b, d, slot):
        copies = [pltpu.make_async_copy(y_ref.at[slot, r], made_hbm.at[b * TURNS + r, d], y_sem.at[slot, r]) for r in range(TURNS)]
        for copy in copies:
            copy.start()
        for copy in copies:
            copy.wait()

    def near_tile(b):
        copies = []
        for r in range(TURNS):
            for n, (src, place) in enumerate(go(b * TURNS + r).kept()):
                copies.append(pltpu.make_async_copy(src, x_ref.at[(b, r, *place[1:])], x_sem.at[b, 3 * r + n]))
        for copy in copies:
            copy.start()
        for copy in copies:
            copy.wait()
        inner_part(b)
        down_part(b)
        put(b, 0, b)

    def far_of(s):
        j = lax.rem(s, 3)
        return s // 3, j, 1 + 2 * j - 3 * (j // 2)

    def far_loads(s, slot):
        b, _, d = far_of(s)
        return [pltpu.make_async_copy(go(b * TURNS + r).last.at[d - 1], x_ref.at[slot, r], x_sem.at[slot, r]) for r in range(TURNS)]

    def begin(s, slot):
        b, _, d = far_of(s)
        for r in range(TURNS):
            go(b * TURNS + r).wait_last(d)
        for copy in far_loads(s, slot):
            copy.start()

    def far_tile(s):
        slot = lax.rem(s, 2)
        b, j, d = far_of(s)

        @pl.when(j == 0)
        def _():
            begin(s, slot)

        for copy in far_loads(s, slot):
            copy.wait()
        inner_part(slot)

        @pl.when(j < 2)
        def _():
            begin(s + 1, 1 - slot)

        down_part(slot)
        put(b, d, slot)
        for r in range(TURNS):
            come(b * TURNS + r).push(0, d)

        @pl.when(s == 4)
        def _():
            each(0, TURNS, lambda u: advance(come(u), 0))

    near_tile(0)
    each(TURNS, n_units, lambda u: advance(go(u), 1))
    near_tile(1)
    each(0, n_units, far_tile)
    each(0, TURNS, lambda u: advance(come(u), 1))
    each(TURNS, n_units, lambda u: advance(come(u), 0))
    each(TURNS, n_units, lambda u: advance(come(u), 1))

    def loads(exchange, slot):
        pieces = [(exchange.last, (pl.ds(1, 3),))] + exchange.kept()
        return [pltpu.make_async_copy(src, x_ref.at[(slot, *place)], x_sem.at[slot, n]) for n, (src, place) in enumerate(pieces)]

    def fetch(exchange, slot):
        for d in range(1, RING):
            exchange.wait_last(d)
        for copy in loads(exchange, slot):
            copy.start()

    fetch(come(0), 0)

    def mix(u):
        slot = lax.rem(u, 2)
        for c in range(rows // 128):
            at = lax.broadcasted_iota(jnp.int32, (128, n_tokens), 0) + (u * rows + c * 128)
            part = jnp.zeros((128, n_tokens), jnp.float32)
            for k in range(top_k):
                part += jnp.where(place_ref[k:k + 1, :] == at, weight_ref[k:k + 1, :], 0.0)
            mix_ref[:, c * 128:(c + 1) * 128] = part.T.astype(jnp.bfloat16)
        for copy in loads(come(u), slot):
            copy.wait()

        @pl.when(u + 1 < n_units)
        def _():
            fetch(come(u + 1), 1 - slot)

        x2 = x_ref.at[slot].reshape(rows, 2 * half)

        def mix_step(n, carry):
            total_ref[:, block_at(n)] += dot32(mix_ref[...], x2[:, block_at(n)])
            return carry

        lax.fori_loop(0, 2 * half // WIDE, mix_step, 0)

    each(0, n_units, mix)
    sum_ref[...] = total_ref[...].astype(jnp.bfloat16)
    for copy in far_weights:
        copy.wait_send()

    def pair_done(n, carry):
        for copy in shared_push(n):
            copy.wait_send()
        return carry

    lax.fori_loop(0, n_shared, pair_done, 0)

    def sent(u):
        go(u).wait_sent()
        come(u).wait_sent()

    each(0, n_units, sent)


def moe_exchange(n_units, normed, hidden, place, weight, weights, shared):
    n_tokens, width = normed.shape
    anywhere = pl.BlockSpec(memory_space=pl.ANY)
    vmem = pl.BlockSpec(memory_space=pltpu.VMEM)
    inner, n_shared = weights[0].shape[1], shared[0].shape[1] // WIDE

    def blocks(*lead):
        return jax.ShapeDtypeStruct((n_units, *lead, BLOCK, width), jnp.bfloat16)

    cube = (RING, RING, RING, BLOCK, width)
    steps = [blocks(4, 4, 3), blocks(4, 3, 4), blocks(3, 4, 4)]
    wide_block = jax.ShapeDtypeStruct((n_shared, width // 2, WIDE), jnp.bfloat16)
    far = [wide_block, wide_block, jax.ShapeDtypeStruct(shared[2].shape, jnp.bfloat16)]
    outs = [jax.ShapeDtypeStruct((n_tokens, width), jnp.bfloat16)] + far + [blocks(4, 4, 4)] + steps + [blocks(4, 4, 4)] + steps
    sems = pltpu.SemaphoreType.DMA
    return pl.pallas_call(
        functools.partial(moe_kernel, n_units),
        out_shape=tuple(outs),
        in_specs=[vmem] * 4 + [anywhere] * 6,
        out_specs=(vmem,) + (anywhere,) * 11,
        scratch_shapes=[pltpu.VMEM(w.shape, jnp.bfloat16) for w in weights for _ in range(2)] + [
            pltpu.VMEM((2, 4, width // 2, WIDE), jnp.bfloat16),
            pltpu.VMEM((2, 2, WIDE, width // 2), jnp.bfloat16),
            pltpu.VMEM((2, *cube), jnp.bfloat16),
            pltpu.VMEM((RING ** 3 * BLOCK, inner), jnp.bfloat16),
            pltpu.VMEM((2, TURNS, *cube[1:]), jnp.bfloat16),
            pltpu.VMEM((n_tokens, width), jnp.float32),
            pltpu.VMEM((n_tokens, RING ** 3 * BLOCK), jnp.bfloat16),
            pltpu.VMEM((RING ** 3 * BLOCK, n_tokens), jnp.bfloat16),
            sems((3,)), sems((3, n_shared)), sems((3, n_shared)), sems((3,)), sems((3,)), sems((2, 6)), sems((2, 9)), sems((2, 3)),
            sems((n_units, 5)), sems((n_units, 5)), sems((n_units, 5)), sems((n_units, 5)),
        ],
        compiler_params=pltpu.CompilerParams(collective_id=0, has_side_effects=True, vmem_limit_bytes=60 * 1024 * 1024),
        cost_estimate=pl.CostEstimate(flops=250_000_000_000, bytes_accessed=100_000_000, transcendentals=0),
        name="moe_exchange",
    )(normed, hidden, place, weight, *weights, *shared)[0]


def solution(mesh):
    n_ep = mesh.shape["ep"]
    tok_spec = P(("data", "fsdp", "ep"))
    row_spec = P("fsdp", None)

    def local_step(x_in, w_qkv, w_out, w_gate, w_up, w_down, ws_gate, ws_up, ws_down, expert_ids, slot_ids, gate_vals):
        n_batch, seq_len, model_dim = x_in.shape
        n_tokens = n_batch * seq_len
        top_k = expert_ids.shape[-1]
        n_experts = w_gate.shape[0] * n_ep
        capacity = capacity_for(n_tokens, top_k, n_experts)
        ids_flat = expert_ids.reshape(n_tokens, top_k).T
        slots_flat = slot_ids.reshape(n_tokens, top_k).T
        me = lax.axis_index("ep")
        rel = [lax.rem(ids_flat // s - me // s + n_ep, RING) for s in STRIDES]
        unit, within = slots_flat // BLOCK, slots_flat % BLOCK
        turn = unit % TURNS
        place = jnp.zeros_like(slots_flat)
        for r in range(TURNS):
            order = [rel[(r + k) % 3] for k in range(3)]
            place = jnp.where(turn == r, (order[0] * RING + order[1]) * RING + order[2], place)
        row_of = jnp.where(slots_flat >= 0, (unit * n_experts + place) * BLOCK + within, -1)
        gates = gate_vals.reshape(n_tokens, top_k).T.astype(jnp.float32)
        hidden, normed = attention(x_in.reshape(n_tokens, model_dim), w_qkv, w_out)
        summed = moe_exchange(capacity // BLOCK, normed, hidden, row_of, gates, (w_gate[0], w_up[0], w_down[0]), (ws_gate, ws_up, ws_down))
        return summed.reshape(n_batch, seq_len, model_dim)

    return jax.shard_map(local_step, mesh=mesh, in_specs=(tok_spec, row_spec, row_spec, P("ep", "fsdp", None), P("ep", "fsdp", None), P("ep", None, "fsdp"), row_spec, row_spec, P(None, "fsdp"), tok_spec, tok_spec, tok_spec), out_specs=tok_spec, check_vma=False)
```
